32 devices in a mesh: dp: 2 (over x), emb: 4 (over z), head: 4 (over y, core).
Axes of the slice: x: 2, y: 2, z: 4, core: 2. Of those that a mesh axis runs over, the one named last changes fastest.
Arguments:
- hidden: bfloat16 [64, 128, 5120], P('dp', None, 'emb'), parts along dimension 0
- g_in: bfloat16 [5120], P('emb')
- w_dq: bfloat16 [5120, 1536], P('emb', 'head')
- g_q: bfloat16 [1536], P('head')
- w_dkv: bfloat16 [5120, 512], P('emb', 'head')
- g_kv: bfloat16 [512], P('head')
- w_kr: bfloat16 [5120, 64], P('emb')
- w_uq: bfloat16 [1536, 128, 192], P(None, 'head')
- w_uk: bfloat16 [512, 128, 128], P(None, 'head')
- w_uv: bfloat16 [512, 128, 128], P(None, 'head')
- w_o: bfloat16 [128, 128, 5120], P('head', None, 'emb')
Outputs:
- output 1: bfloat16 [64, 128, 5120], P('dp', None, 'emb'), parts along dimension 0
- output 2: bfloat16 [64, 128, 512], P('dp', None, 'head'), parts along dimension 0
- output 3: bfloat16 [64, 128, 64], P('dp'), parts along dimension 0
There are 2 independent parts. The reference program is written for one: setup_inputs(seed, part) draws one part's arguments, and reference() takes and returns one part's arrays. A program takes and returns all parts, laid end to end along the dimension named above; an argument that names none is the same for every part.
All inputs are finite; a program needn't handle non-finite values.
Results may differ from the reference program's by a relative error of at most 0.02.
Values are sent between devices in bfloat16 or wider.
A program may use at most 1 GiB of HBM per device.

```python
import math
import jax
import jax.numpy as jnp
from jax import lax

BATCH = 32
SEQ = 128
D = 5120
HEADS = 128
Q_LORA = 1536
KV_LORA = 512
NOPE = 128
ROPE = 64
VDIM = 128

QK_DIM = NOPE + ROPE
HALF_ROPE = ROPE // 2
Q_BLOCK = min(SEQ, 128)
BLOCKS_PER_SEQ = SEQ // Q_BLOCK
NUM_BLOCKS = BATCH * BLOCKS_PER_SEQ
ROPE_BASE = 10000.0
NORM_EPS = 1.0e-6
MSCALE = 0.1 * math.log(40.0) + 1.0
SOFTMAX_SCALE = MSCALE * MSCALE / math.sqrt(QK_DIM)


def setup_inputs(seed: int = 0, part: int = 0) -> dict:
    key_list = jax.random.split(jax.random.key(seed), 10)
    part_key = jax.random.fold_in(jax.random.key(seed + 1), part)

    def make_gain(sub_key, count):
        return jax.random.uniform(sub_key, (count,), jnp.float32, 0.5, 1.5).astype(jnp.bfloat16)

    def weight(sub_key, arr_shape, fan_in):
        return (jax.random.normal(sub_key, arr_shape, jnp.float32) * fan_in ** -0.5).astype(jnp.bfloat16)

    hidden = 0.5 * jax.random.normal(part_key, (BATCH, SEQ, D), jnp.float32)
    return {
        "hidden": hidden.astype(jnp.bfloat16),
        "g_in": make_gain(key_list[0], D),
        "w_dq": weight(key_list[1], (D, Q_LORA), D),
        "g_q": make_gain(key_list[2], Q_LORA),
        "w_dkv": weight(key_list[3], (D, KV_LORA), D),
        "g_kv": make_gain(key_list[4], KV_LORA),
        "w_kr": weight(key_list[5], (D, ROPE), D),
        "w_uq": weight(key_list[6], (Q_LORA, HEADS, QK_DIM), Q_LORA),
        "w_uk": weight(key_list[7], (KV_LORA, HEADS, NOPE), KV_LORA),
        "w_uv": weight(key_list[8], (KV_LORA, HEADS, VDIM), KV_LORA),
        "w_o": weight(key_list[9], (HEADS, VDIM, D), HEADS * VDIM),
    }


def rms_norm(values, gain_vec):
    wide_vals = values.astype(jnp.float32)
    mean_sq = jnp.mean(wide_vals * wide_vals, axis=-1, keepdims=True)
    return (wide_vals * lax.rsqrt(mean_sq + NORM_EPS) * gain_vec.astype(jnp.float32)).astype(jnp.bfloat16)


def rope_tables():
    inv_freq = ROPE_BASE ** (-2.0 * jnp.arange(HALF_ROPE, dtype=jnp.float32) / ROPE)
    angles = jnp.arange(SEQ, dtype=jnp.float32)[:, None] * inv_freq[None, :]
    return jnp.cos(angles), jnp.sin(angles)


def rotate(values, cos_t, sin_t):
    front_half = values[..., :HALF_ROPE]
    back_half = values[..., HALF_ROPE:]
    return jnp.concatenate([front_half * cos_t - back_half * sin_t, front_half * sin_t + back_half * cos_t], axis=-1)


def reference(hidden, g_in, w_dq, g_q, w_dkv, g_kv, w_kr, w_uq, w_uk, w_uv, w_o):
    tokens = rms_norm(hidden, g_in).reshape(BATCH * SEQ, D)
    c_q = jnp.dot(tokens, w_dq, preferred_element_type=jnp.float32).astype(jnp.bfloat16)
    c_kv = jnp.dot(tokens, w_dkv, preferred_element_type=jnp.float32).astype(jnp.bfloat16)
    k_raw = jnp.dot(tokens, w_kr, preferred_element_type=jnp.float32).astype(jnp.bfloat16)
    cq_norm = rms_norm(c_q, g_q)
    ckv_norm = rms_norm(c_kv, g_kv)
    cos_t, sin_t = rope_tables()
    k_pe = rotate(k_raw.reshape(BATCH, SEQ, ROPE).astype(jnp.float32), cos_t, sin_t).astype(jnp.bfloat16)
    q_all = jnp.dot(cq_norm, w_uq.reshape(Q_LORA, HEADS * QK_DIM), preferred_element_type=jnp.float32)
    q_all = q_all.astype(jnp.bfloat16).reshape(BATCH, SEQ, HEADS, QK_DIM)
    q_nope = q_all[..., :NOPE]
    q_pe = rotate(q_all[..., NOPE:].astype(jnp.float32), cos_t[:, None, :], sin_t[:, None, :]).astype(jnp.bfloat16)
    k_nope = jnp.dot(ckv_norm, w_uk.reshape(KV_LORA, HEADS * NOPE), preferred_element_type=jnp.float32)
    k_nope = k_nope.astype(jnp.bfloat16).reshape(BATCH, SEQ, HEADS, NOPE)
    v_heads = jnp.dot(ckv_norm, w_uv.reshape(KV_LORA, HEADS * VDIM), preferred_element_type=jnp.float32)
    v_heads = v_heads.astype(jnp.bfloat16).reshape(BATCH, SEQ, HEADS, VDIM)
    key_pos = jnp.arange(SEQ)

    def attend_block(blk_idx):
        seq_idx = blk_idx // BLOCKS_PER_SEQ
        q_start = (blk_idx % BLOCKS_PER_SEQ) * Q_BLOCK
        qn_seq = lax.dynamic_index_in_dim(q_nope, seq_idx, 0, keepdims=False)
        qp_seq = lax.dynamic_index_in_dim(q_pe, seq_idx, 0, keepdims=False)
        qn_blk = lax.dynamic_slice_in_dim(qn_seq, q_start, Q_BLOCK, 0).astype(jnp.float32)
        qp_blk = lax.dynamic_slice_in_dim(qp_seq, q_start, Q_BLOCK, 0).astype(jnp.float32)
        kn_seq = lax.dynamic_index_in_dim(k_nope, seq_idx, 0, keepdims=False).astype(jnp.float32)
        kp_seq = lax.dynamic_index_in_dim(k_pe, seq_idx, 0, keepdims=False).astype(jnp.float32)
        v_seq = lax.dynamic_index_in_dim(v_heads, seq_idx, 0, keepdims=False).astype(jnp.float32)
        scores = jnp.einsum("qhd,khd->hqk", qn_blk, kn_seq) + jnp.einsum("qhr,kr->hqk", qp_blk, kp_seq)
        q_pos = q_start + jnp.arange(Q_BLOCK)
        allowed = key_pos[None, :] <= q_pos[:, None]
        scores = jnp.where(allowed[None, :, :], scores * SOFTMAX_SCALE, -jnp.inf)
        attn_prob = jax.nn.softmax(scores, axis=-1).astype(jnp.bfloat16).astype(jnp.float32)
        return jnp.einsum("hqk,khv->qhv", attn_prob, v_seq).astype(jnp.bfloat16)

    context = lax.map(attend_block, jnp.arange(NUM_BLOCKS)).reshape(BATCH * SEQ, HEADS * VDIM)
    attn_sum = jnp.dot(context, w_o.reshape(HEADS * VDIM, D), preferred_element_type=jnp.float32)
    result = (hidden.astype(jnp.float32) + attn_sum.reshape(BATCH, SEQ, D)).astype(jnp.bfloat16)
    return (result, ckv_norm.reshape(BATCH, SEQ, KV_LORA), k_pe)
```

```python
import functools
import math
import jax
import jax.numpy as jnp
from jax import lax
from jax.experimental import pallas as pl
from jax.experimental.pallas import tpu as pltpu
from jax.sharding import PartitionSpec as P

ROPE_BASE = 10000.0
NORM_EPS = 1.0e-6
MSCALE = 0.1 * math.log(40.0) + 1.0
LOG2E = math.log2(math.e)
GH = 4
BS = 4
NT = (((1,), (1,)), ((), ()))


def split_norm(latent, gain_vec, full_width, axis_name):
    wide_vals = latent.astype(jnp.float32)
    sq_sum = lax.psum(jnp.sum(wide_vals * wide_vals, axis=-1, keepdims=True), axis_name)
    return (wide_vals * lax.rsqrt(sq_sum / full_width + NORM_EPS) * gain_vec.astype(jnp.float32)).astype(jnp.bfloat16)


def rope_tables(seq_len, rope_dim):
    half_dim = rope_dim // 2
    inv_freq = ROPE_BASE ** (-2.0 * jnp.arange(half_dim, dtype=jnp.float32) / rope_dim)
    angles = jnp.arange(seq_len, dtype=jnp.float32)[:, None] * inv_freq[None, :]
    return jnp.cos(angles), jnp.sin(angles)


def rotate(values, cos_t, sin_t):
    half_dim = values.shape[-1] // 2
    front_half = values[..., :half_dim]
    back_half = values[..., half_dim:]
    return jnp.concatenate([front_half * cos_t - back_half * sin_t, front_half * sin_t + back_half * cos_t], axis=-1)


def attn_kernel(scale, cq_ref, ckv_ref, kp_ref, rope_ref, wq_hbm, wkv_hbm, wo_hbm, out_ref, wq, wkv, wo, ctx, wsem, osem):
    first = pl.program_id(0) == 0
    groups = wq.shape[0]
    seq = rope_ref.shape[0]
    toks = cq_ref.shape[0]
    seqs = toks // seq

    @pl.when(first)
    def _():
        for g in range(groups):
            pltpu.make_async_copy(wq_hbm.at[g], wq.at[g], wsem.at[0, g]).start()
            pltpu.make_async_copy(wkv_hbm.at[g], wkv.at[g], wsem.at[1, g]).start()
        pltpu.make_async_copy(wo_hbm, wo, osem).start()

    lane = lax.broadcasted_iota(jnp.int32, (seq, 128), 1)
    low = (lane & 63) < 32
    causal = lax.broadcasted_iota(jnp.int32, (seq, seq), 0) >= lax.broadcasted_iota(jnp.int32, (seq, seq), 1)

    def group(g, carry):
        @pl.when(first)
        def _():
            pltpu.make_async_copy(wq_hbm.at[g], wq.at[g], wsem.at[0, g]).wait()
            pltpu.make_async_copy(wkv_hbm.at[g], wkv.at[g], wsem.at[1, g]).wait()

        q = jnp.dot(cq_ref[...], wq[g], preferred_element_type=jnp.float32).astype(jnp.bfloat16)
        kv = jnp.dot(ckv_ref[...], wkv[g], preferred_element_type=jnp.float32).astype(jnp.bfloat16)
        for s in range(seqs):
            rows = slice(s * seq, (s + 1) * seq)
            cos_t = rope_ref[:, 0:128]
            sin_t = rope_ref[:, 128:256]
            qps = []
            for t in range(GH // 2):
                u = q[rows, GH * 128 + t * 128:GH * 128 + (t + 1) * 128].astype(jnp.float32)
                swapped = jnp.where(low, pltpu.roll(u, 96, 1), pltpu.roll(u, 32, 1))
                qps.append((u * cos_t + swapped * sin_t).astype(jnp.bfloat16))
            for i in range(GH):
                q_cat = jnp.concatenate([q[rows, i * 128:(i + 1) * 128], qps[i // 2]], axis=1)
                k_cat = jnp.concatenate([kv[rows, i * 128:(i + 1) * 128], kp_ref[rows, (i % 2) * 128:(i % 2 + 1) * 128]], axis=1)
                sc = lax.dot_general(q_cat, k_cat, NT, preferred_element_type=jnp.float32)
                sc = jnp.where(causal, sc, -jnp.inf)
                top = jnp.max(sc, axis=1, keepdims=True)
                e = jnp.exp2((sc - top) * (scale * LOG2E))
                p = (e * (1.0 / jnp.sum(e, axis=1, keepdims=True))).astype(jnp.bfloat16)
                o = jnp.dot(p, kv[rows, (GH + i) * 128:(GH + i + 1) * 128], preferred_element_type=jnp.float32)
                ctx[pl.ds(s * seq, seq), pl.ds(pl.multiple_of(g * (GH * 128) + i * 128, 128), 128)] = o.astype(jnp.bfloat16)
        return carry

    lax.fori_loop(0, groups, group, 0)

    @pl.when(first)
    def _():
        pltpu.make_async_copy(wo_hbm, wo, osem).wait()

    out_ref[...] = jnp.dot(ctx[...], wo[...], preferred_element_type=jnp.float32).astype(jnp.bfloat16)


def attention(cq, ckv, kp, rope, wq, wkv, wo, scale, seq):
    toks, cq_dim = cq.shape
    width = wo.shape[1]
    block = BS * seq
    whole = lambda: pl.BlockSpec(memory_space=pl.ANY)
    return pl.pallas_call(
        functools.partial(attn_kernel, scale),
        grid=(toks // block,),
        out_shape=jax.ShapeDtypeStruct((toks, width), jnp.bfloat16),
        in_specs=[
            pl.BlockSpec((block, cq_dim), lambda b: (b, 0)),
            pl.BlockSpec((block, ckv.shape[1]), lambda b: (b, 0)),
            pl.BlockSpec((block, kp.shape[1]), lambda b: (b, 0)),
            pl.BlockSpec(rope.shape, lambda b: (0, 0)),
            whole(), whole(), whole(),
        ],
        out_specs=pl.BlockSpec((block, width), lambda b: (b, 0)),
        scratch_shapes=[
            pltpu.VMEM(wq.shape, jnp.bfloat16),
            pltpu.VMEM(wkv.shape, jnp.bfloat16),
            pltpu.VMEM(wo.shape, jnp.bfloat16),
            pltpu.VMEM((block, wo.shape[0]), jnp.bfloat16),
            pltpu.SemaphoreType.DMA((2, wq.shape[0])),
            pltpu.SemaphoreType.DMA,
        ],
        compiler_params=pltpu.CompilerParams(dimension_semantics=("arbitrary",), vmem_limit_bytes=67_000_000),
        cost_estimate=pl.CostEstimate(flops=171_000_000_000, bytes_accessed=70_000_000, transcendentals=17_000_000),
        name="mla_attention",
    )(cq, ckv, kp, rope, wq, wkv, wo)


def pack_weights(w_uq, w_uk, w_uv, w_o):
    cdim, heads, qk = w_uq.shape
    nope = w_uk.shape[2]
    groups = heads // GH
    qn = w_uq[:, :, :nope].reshape(cdim, groups, GH * nope)
    qr = w_uq[:, :, nope:].reshape(cdim, groups, GH * (qk - nope))
    wq = jnp.concatenate([qn, qr], axis=2).transpose(1, 0, 2)
    k = w_uk.reshape(w_uk.shape[0], groups, GH * nope)
    v = w_uv.reshape(w_uv.shape[0], groups, GH * w_uv.shape[2])
    wkv = jnp.concatenate([k, v], axis=2).transpose(1, 0, 2)
    return wq, wkv, w_o.reshape(heads * w_o.shape[1], w_o.shape[2])


def solution(mesh):
    emb_count = mesh.shape["emb"]
    in_specs = (P("dp", None, "emb"), P("emb"), P("emb", "head"), P("head"), P("emb", "head"), P("head"), P("emb", None), P(None, "head", None), P(None, "head", None), P(None, "head", None), P("head", None, "emb"))
    out_specs = (P("dp", None, "emb"), P("dp", None, "head"), P("dp", None, None))

    def local_block(hidden, g_in, w_dq, g_q, w_dkv, g_kv, w_kr, w_uq, w_uk, w_uv, w_o):
        nseq, seq_len = hidden.shape[:2]
        soft_scale = MSCALE * MSCALE / math.sqrt(w_uq.shape[2])
        h_norm = split_norm(hidden, g_in, hidden.shape[2] * emb_count, "emb")
        cq_part = jnp.einsum("btd,dc->btc", h_norm, w_dq, preferred_element_type=jnp.float32).astype(jnp.bfloat16)
        ckv_part = jnp.einsum("btd,dc->btc", h_norm, w_dkv, preferred_element_type=jnp.float32).astype(jnp.bfloat16)
        kr_part = jnp.einsum("btd,dc->btc", h_norm, w_kr, preferred_element_type=jnp.float32).astype(jnp.bfloat16)
        c_q, c_kv, k_raw = lax.psum((cq_part, ckv_part, kr_part), "emb")
        cq_loc = split_norm(c_q, g_q, w_uq.shape[0], "head")
        ckv_loc = split_norm(c_kv, g_kv, w_uk.shape[0], "head")
        cq_full = lax.all_gather(cq_loc, "head", axis=2, tiled=True)
        ckv_full = lax.all_gather(ckv_loc, "head", axis=2, tiled=True)
        cos_t, sin_t = rope_tables(seq_len, w_kr.shape[1])
        k_pe = rotate(k_raw.astype(jnp.float32), cos_t, sin_t).astype(jnp.bfloat16)
        rope = jnp.concatenate([jnp.tile(cos_t, (1, 4)), jnp.tile(jnp.concatenate([-sin_t, sin_t], axis=1), (1, 2))], axis=1)
        zeros = jnp.zeros_like(k_pe)
        kp = jnp.concatenate([k_pe, zeros, zeros, k_pe], axis=2)
        wq, wkv, wo = pack_weights(w_uq, w_uk, w_uv, w_o)
        toks = nseq * seq_len
        attn_part = attention(
            cq_full.reshape(toks, -1), ckv_full.reshape(toks, -1), kp.reshape(toks, -1), rope, wq, wkv, wo, soft_scale, seq_len
        )
        attn_sum = lax.psum(attn_part.reshape(hidden.shape), "head")
        result = (hidden.astype(jnp.float32) + attn_sum.astype(jnp.float32)).astype(jnp.bfloat16)
        return result, ckv_loc, k_pe

    return jax.shard_map(local_block, mesh=mesh, in_specs=in_specs, out_specs=out_specs, check_vma=False)
```

```python
import functools
import math
import jax
import jax.numpy as jnp
from jax import lax
from jax.experimental import pallas as pl
from jax.experimental.pallas import tpu as pltpu
from jax.sharding import PartitionSpec as P

ROPE_BASE = 10000.0
NORM_EPS = 1.0e-6
MSCALE = 0.1 * math.log(40.0) + 1.0
LOG2E = math.log2(math.e)
GH = 4
BS = 2
LEAD = 5
RING = 8
NT = (((1,), (1,)), ((), ()))
F32 = jnp.float32
BF16 = jnp.bfloat16


def rope_tables(seq_len, rope_dim):
    half_dim = rope_dim // 2
    inv_freq = ROPE_BASE ** (-2.0 * jnp.arange(half_dim, dtype=F32) / rope_dim)
    angles = jnp.arange(seq_len, dtype=F32)[:, None] * inv_freq[None, :]
    return jnp.cos(angles), jnp.sin(angles)


def kernel(
    dims,
    h_hbm, ssq, g_in, gains, rope, rope_t, wd_hbm, wq_hbm, wk_hbm, wv_hbm, wo_hbm,
    out_hbm, ckv_hbm, kpe_hbm, latz, lath,
    wd, wq, wk, wv, wo, qa, ka, va, qb, kb, vb, ctx, cqn, ckvn, lato, latn,
    hbuf, part, rsr, cz, o1s, own, o2s, fin, hres, o1r, o2r, cko, kpo, ssr, gnr, rall,
    wsem, hsem, ssem, gsem, rs_s, rs_r, ag_s, ag_r, ag_l, y_s, y_r, d_s, d_r, f_s, f_r,
    ld, o1_s, o1_r, o2_s, o2_r, o3_s, o3_r, o3_l, hr, cko_l, kpo_l,
):
    nb, seq, nz, d_model, q_lora, kv_lora, scale = dims
    blk = BS * seq
    piece = blk // nz
    groups = wq.shape[0]
    width = h_hbm.shape[1]
    half = width // 2
    qc, kc = q_lora // 4, kv_lora // 4
    lat = qc + kc
    rd = kpe_hbm.shape[1]
    z = lax.axis_index("emb")
    head = lax.axis_index("head")
    core = head % 2
    partner = head + 1 - 2 * core
    ypeer = (head + 2) % 4
    diag = (partner + 2) % 4
    others = (partner, ypeer, diag)

    def remote(src, dst, ss, rs, **where):
        return pltpu.make_async_remote_copy(
            src_ref=src, dst_ref=dst, send_sem=ss, recv_sem=rs, device_id=where, device_id_type=pl.DeviceIdType.MESH
        )

    def rows(b):
        return pl.ds(pl.multiple_of(b * blk, blk), blk)

    def zt(d):
        return (z + d) % nz

    def ss_copy(d):
        return remote(ssq, ssr.at[d - 1], ssem.at[0, d - 1], ssem.at[1, d - 1], emb=zt(d))

    def gn_copy(r):
        return remote(gains, gnr.at[r], gsem.at[0, r], gsem.at[1, r], head=others[r])

    def h_copy(b):
        return pltpu.make_async_copy(h_hbm.at[rows(b)], hbuf.at[b % 2], hsem.at[b % 2])

    def rs_copy(b, d):
        src = part.at[b % 2, pl.ds(pl.multiple_of(zt(d) * piece, piece), piece)]
        return remote(src, rsr.at[b % RING, d - 1], rs_s.at[b, d - 1], rs_r.at[b, d - 1], emb=zt(d))

    def own_rows(b):
        return pl.ds(pl.multiple_of(b * blk + z * piece, piece), piece)

    def ag_copy(b, d):
        return remote(cz.at[b % 2], latz.at[own_rows(b)], ag_s.at[b, d - 1], ag_r.at[b, d - 1], emb=zt(d))

    def ag_local(b):
        return pltpu.make_async_copy(cz.at[b % 2], latz.at[own_rows(b)], ag_l.at[b % 2])

    def y_copy(b):
        return remote(latz.at[rows(b), pl.ds(0, lat)], lath.at[1, rows(b)], y_s.at[b], y_r.at[b], head=ypeer)

    def d_copy(b):
        return remote(latz.at[rows(b), pl.ds(0, lat)], lath.at[0, rows(b)], d_s.at[b], d_r.at[b], head=partner)

    def f_copy(b):
        return remote(lath.at[1, rows(b)], lath.at[2, rows(b)], f_s.at[b], f_r.at[b], head=partner)

    def loads(b):
        return [pltpu.make_async_copy(latz.at[rows(b)], lato, ld.at[0])] + [
            pltpu.make_async_copy(lath.at[r, rows(b)], latn.at[r], ld.at[1 + r]) for r in range(3)
        ]

    def o1_copy(b):
        return remote(o1s.at[b % 2], o1r.at[b % RING], o1_s.at[b], o1_r.at[b], head=partner)

    def o2_copy(b):
        return remote(o2s.at[b % 2], o2r.at[b % RING], o2_s.at[b], o2_r.at[b], head=ypeer)

    def my_half():
        return pl.ds(pl.multiple_of(core * half, half), half)

    def o3_copy(b):
        return remote(fin.at[b % 2], out_hbm.at[rows(b), my_half()], o3_s.at[b], o3_r.at[b], head=partner)

    def o3_local(b):
        return pltpu.make_async_copy(fin.at[b % 2], out_hbm.at[rows(b), my_half()], o3_l.at[b % 2])

    def hr_copy(b):
        return pltpu.make_async_copy(h_hbm.at[rows(b), my_half()], hres.at[b % 2], hr.at[b % 2])

    def cko_copy(b):
        return pltpu.make_async_copy(cko.at[b % 2], ckv_hbm.at[rows(b)], cko_l.at[b % 2])

    def kpo_copy(b):
        return pltpu.make_async_copy(kpo.at[b % 2], kpe_hbm.at[rows(b)], kpo_l.at[b % 2])

    mine = pl.ds(pl.multiple_of(core * half, half), half)
    theirs = pl.ds(pl.multiple_of((1 - core) * half, half), half)
    weight_copies = [
        pltpu.make_async_copy(wd_hbm, wd, wsem.at[0]),
        pltpu.make_async_copy(wq_hbm, wq, wsem.at[1]),
        pltpu.make_async_copy(wk_hbm, wk, wsem.at[2]),
        pltpu.make_async_copy(wv_hbm, wv, wsem.at[3]),
        pltpu.make_async_copy(wo_hbm.at[mine], wo.at[pl.ds(0, half)], wsem.at[4]),
        pltpu.make_async_copy(wo_hbm.at[theirs], wo.at[pl.ds(half, half)], wsem.at[5]),
    ]
    weight_copies[0].start()
    h_copy(0).start()

    barrier = pltpu.get_barrier_semaphore()
    for d in range(1, nz):
        pl.semaphore_signal(barrier, inc=1, device_id={"emb": zt(d)}, device_id_type=pl.DeviceIdType.MESH)
    for other in others:
        pl.semaphore_signal(barrier, inc=1, device_id={"head": other}, device_id_type=pl.DeviceIdType.MESH)
    pl.semaphore_wait(barrier, nz - 1 + 3)

    for d in range(1, nz):
        ss_copy(d).start()
    for r in range(3):
        gn_copy(r).start()
    for copy in weight_copies[1:]:
        copy.start()
    weight_copies[0].wait()
    total = ssq[...]
    for d in range(1, nz):
        ss_copy(d).wait()
        total = total + ssr[d - 1]
    rall[...] = lax.rsqrt(total / d_model + NORM_EPS)

    def down(b):
        h_copy(b).wait()

        @pl.when(b + 1 < nb)
        def _():
            h_copy(b + 1).start()

        @pl.when(b >= 2)
        def _():
            for d in range(1, nz):
                rs_copy(b - 2, d).wait_send()

        for s in range(BS):
            stat = jnp.transpose(jnp.broadcast_to(rall[pl.ds(b * BS + s, 1), :], (seq, seq)))[:, 0:1]
            x = hbuf[b % 2, s * seq:(s + 1) * seq, :].astype(F32)
            hn = (x * stat * g_in[0:1, :]).astype(BF16)
            part[b % 2, s * seq:(s + 1) * seq, :] = jnp.dot(hn, wd[...], preferred_element_type=F32).astype(BF16)
        for d in range(1, nz):
            rs_copy(b, d).start()

    def reduce_z(b):
        for d in range(1, nz):
            rs_copy(b, d).wait_recv()
        acc = part[b % 2, pl.ds(pl.multiple_of(z * piece, piece), piece), :].astype(F32)
        for d in range(1, nz):
            acc = acc + rsr[b % RING, d - 1].astype(F32)

        @pl.when(b >= 2)
        def _():
            for d in range(1, nz):
                ag_copy(b - 2, d).wait_send()

        cz[b % 2] = acc.astype(BF16)
        for d in range(1, nz):
            ag_copy(b, d).start()
        ag_local(b).start()

    def spread(b):
        for d in range(1, nz):
            ag_copy(b, d).wait_recv()
        ag_local(b).wait()
        y_copy(b).start()
        d_copy(b).start()

    def forward(b):
        y_copy(b).wait_recv()
        f_copy(b).start()

    def fetch(b):
        d_copy(b).wait_recv()
        f_copy(b).wait_recv()
        y_copy(b).wait_send()
        d_copy(b).wait_send()
        f_copy(b).wait_send()
        for copy in loads(b):
            copy.start()

    def normalize(b):
        for copy in loads(b):
            copy.wait()

        @pl.when(b >= 2)
        def _():
            cko_copy(b - 2).wait()
            kpo_copy(b - 2).wait()

        @pl.when(b == 0)
        def _():
            for r in range(3):
                gn_copy(r).wait()

        def latent(r, lo, hi):
            return (lato[:, lo:hi] if r == 0 else latn[r - 1, :, lo:hi]).astype(F32)

        def gain(r, lo, hi):
            return gains[0:1, lo:hi] if r == 0 else gnr[r - 1, 0:1, lo:hi]

        order = (head,) + others
        for lo, hi, full, dst in ((0, qc, q_lora, cqn), (qc, lat, kv_lora, ckvn)):
            sq = None
            for r in range(4):
                x = latent(r, lo, hi)
                one = jnp.sum(x * x, axis=1, keepdims=True)
                sq = one if sq is None else sq + one
            stat = lax.rsqrt(sq / full + NORM_EPS)
            for r in range(4):
                y = (latent(r, lo, hi) * stat * gain(r, lo, hi)).astype(BF16)
                dst[:, pl.ds(pl.multiple_of(order[r] * (hi - lo), 128), hi - lo)] = y
                if r == 0 and lo == qc:
                    cko[b % 2] = y
        for s in range(BS):
            u = lato[s * seq:(s + 1) * seq, lat:lat + rd].astype(F32)
            fr, bk = u[:, :rd // 2], u[:, rd // 2:]
            cos_n, sin_n = rope[:, :rd // 2], rope[:, rd // 2:]
            kpo[b % 2, s * seq:(s + 1) * seq, :] = jnp.concatenate(
                [fr * cos_n - bk * sin_n, fr * sin_n + bk * cos_n], axis=1
            ).astype(BF16)
        cko_copy(b).start()
        kpo_copy(b).start()

    causal = lax.broadcasted_iota(jnp.int32, (seq, seq), 0) <= lax.broadcasted_iota(jnp.int32, (seq, seq), 1)

    def project(g, q, k, v):
        q[...] = lax.dot_general(wq[g], cqn[...], NT, preferred_element_type=F32).astype(BF16)
        k[...] = jnp.dot(ckvn[...], wk[g], preferred_element_type=F32).astype(BF16)
        v[...] = lax.dot_general(wv[g], ckvn[...], NT, preferred_element_type=F32).astype(BF16)

    def attend(b, g, q, k, v):
        hr_ = rd // 2
        cos_t, sin_t = rope_t[0:hr_, :], rope_t[hr_:rd, :]
        for s in range(BS):
            cols = slice(s * seq, (s + 1) * seq)
            for i in range(GH):
                base = GH * 128 + i * rd
                fr = q[base:base + hr_, cols].astype(F32)
                bk = q[base + hr_:base + rd, cols].astype(F32)
                q_cat = jnp.concatenate(
                    [q[i * 128:(i + 1) * 128, cols], (fr * cos_t - bk * sin_t).astype(BF16), (fr * sin_t + bk * cos_t).astype(BF16)],
                    axis=0,
                )
                k_cat = jnp.concatenate([k[cols, i * 128:(i + 1) * 128], kpo[b % 2, cols, :]], axis=1)
                sc = jnp.dot(k_cat, q_cat, preferred_element_type=F32)
                sc = jnp.where(causal, sc, -jnp.inf)
                top = jnp.max(sc, axis=0, keepdims=True)
                e = jnp.exp2((sc - top) * (scale * LOG2E))
                p = (e * (1.0 / jnp.sum(e, axis=0, keepdims=True))).astype(BF16)
                o = jnp.dot(v[i * 128:(i + 1) * 128, cols], p, preferred_element_type=F32)
                ctx[pl.ds(pl.multiple_of(g * (GH * 128) + i * 128, 128), 128), cols] = o.astype(BF16)

    def attention(b):
        @pl.when(b == 0)
        def _():
            for copy in weight_copies[1:]:
                copy.wait()

        project(0, qa, ka, va)

        def two(k, carry):
            g = 2 * k
            project(g + 1, qb, kb, vb)
            attend(b, g, qa, ka, va)
            project(g + 2, qa, ka, va)
            attend(b, g + 1, qb, kb, vb)
            return carry

        lax.fori_loop(0, groups // 2 - 1, two, 0)
        project(groups - 1, qb, kb, vb)
        attend(b, groups - 2, qa, ka, va)
        attend(b, groups - 1, qb, kb, vb)

    def out_first(b):
        @pl.when(b >= 2)
        def _():
            o1_copy(b - 2).wait_send()

        o1s[b % 2] = jnp.dot(wo[half:, :], ctx[...], preferred_element_type=F32).astype(BF16)
        o1_copy(b).start()
        own[b % 2] = jnp.dot(wo[:half, :], ctx[...], preferred_element_type=F32)

    def out_second(b):
        o1_copy(b).wait_recv()

        @pl.when(b >= 2)
        def _():
            o2_copy(b - 2).wait_send()

        o2s[b % 2] = (own[b % 2] + o1r[b % RING].astype(F32)).astype(BF16)
        o2_copy(b).start()
        hr_copy(b).start()

    def out_third(b):
        o2_copy(b).wait_recv()
        hr_copy(b).wait()

        @pl.when(b >= 2)
        def _():
            o3_copy(b - 2).wait()
            o3_local(b - 2).wait()

        both = o2s[b % 2].astype(F32) + o2r[b % RING].astype(F32)
        fin[b % 2] = (hres[b % 2].astype(F32) + jnp.transpose(both)).astype(BF16)
        o3_copy(b).start()
        o3_local(b).start()

    def step(n, carry):
        i = n - LEAD

        def stage(fn, b):
            pl.when(jnp.logical_and(b >= 0, b < nb))(lambda: fn(b))

        stage(forward, i + 2)
        stage(spread, i + 3)
        stage(reduce_z, i + 4)
        stage(down, i + 5)
        stage(out_third, i - 2)
        stage(out_second, i - 1)
        stage(normalize, i)
        stage(fetch, i + 1)

        @pl.when(jnp.logical_and(i >= 0, i < nb))
        def _():
            attention(i)
            out_first(i)

        return carry

    lax.fori_loop(0, nb + LEAD + 2, step, 0)

    for b in (nb - 2, nb - 1):
        for d in range(1, nz):
            rs_copy(b, d).wait_send()
            ag_copy(b, d).wait_send()
        o1_copy(b).wait_send()
        o2_copy(b).wait_send()
        o3_copy(b).wait()
        o3_local(b).wait()
        cko_copy(b).wait()
        kpo_copy(b).wait()


def run_kernel(h, ssq, g_in, gains, rope, rope_t, wd, wq, wk, wv, wo, scale, nz, q_lora, kv_lora):
    toks, width = h.shape
    seq = rope.shape[0]
    rd = rope.shape[1]
    nb = toks // (BS * seq)
    blk, half = BS * seq, width // 2
    piece = blk // nz
    lat = q_lora // 4 + kv_lora // 4
    latw = wd.shape[1]
    dims = (nb, seq, nz, width * nz, q_lora, kv_lora, scale)
    dma = lambda *s: pltpu.SemaphoreType.DMA(s)
    vm = lambda *s: pltpu.VMEM(s, BF16)
    vf = lambda *s: pltpu.VMEM(s, F32)
    vmem = pl.BlockSpec(memory_space=pltpu.VMEM)
    anyw = pl.BlockSpec(memory_space=pl.ANY)
    gr = GH * 128
    proj = lambda: [vm(wq.shape[1], blk), vm(blk, gr), vm(gr, blk)]
    shape = jax.ShapeDtypeStruct
    scratch = (
        [vm(*wd.shape), vm(*wq.shape), vm(*wk.shape), vm(*wv.shape), vm(*wo.shape)]
        + proj() + proj()
        + [vm(wo.shape[1], blk), vm(blk, q_lora), vm(blk, kv_lora), vm(blk, latw), vm(3, blk, lat)]
        + [vm(2, blk, width), vm(2, blk, latw), vm(RING, nz - 1, piece, latw), vm(2, piece, latw)]
        + [vm(2, half, blk), vf(2, half, blk), vm(2, half, blk), vm(2, blk, half), vm(2, blk, half)]
        + [vm(RING, half, blk), vm(RING, half, blk), vm(2, blk, kv_lora // 4), vm(2, blk, rd)]
        + [vf(nz - 1, *ssq.shape), vf(3, *gains.shape), vf(*ssq.shape)]
        + [dma(6), dma(2), dma(2, nz - 1), dma(2, 3)]
        + [dma(nb, nz - 1)] * 4 + [dma(2)] + [dma(nb)] * 6
        + [dma(4)] + [dma(nb)] * 6 + [dma(2)] * 4
    )
    return pl.pallas_call(
        functools.partial(kernel, dims),
        out_shape=[
            shape((toks, width), BF16), shape((toks, kv_lora // 4), BF16), shape((toks, rd), BF16),
            shape((toks, latw), BF16), shape((3, toks, lat), BF16),
        ],
        in_specs=[anyw] + [vmem] * 5 + [anyw] * 5,
        out_specs=[anyw] * 5,
        scratch_shapes=scratch,
        compiler_params=pltpu.CompilerParams(collective_id=0, has_side_effects=True, vmem_limit_bytes=67_043_328),
        cost_estimate=pl.CostEstimate(flops=171_000_000_000, bytes_accessed=100_000_000, transcendentals=17_000_000),
        name="mla_block",
    )(h, ssq, g_in, gains, rope, rope_t, wd, wq, wk, wv, wo)


def pack_weights(w_uq, w_uk, w_uv, w_o):
    cdim, heads, qk = w_uq.shape
    kdim, _, nope = w_uk.shape
    groups = heads // GH
    t = w_uq.transpose(1, 2, 0).reshape(groups, GH, qk, cdim)
    wq = jnp.concatenate(
        [t[:, :, :nope].reshape(groups, GH * nope, cdim), t[:, :, nope:].reshape(groups, GH * (qk - nope), cdim)], axis=1
    )
    wk = w_uk.reshape(kdim, groups, GH * nope).transpose(1, 0, 2)
    wv = w_uv.transpose(1, 2, 0).reshape(groups, GH * w_uv.shape[2], kdim)
    wo = w_o.reshape(heads * w_o.shape[1], w_o.shape[2]).T
    return wq, wk, wv, wo


def solution(mesh):
    nz = mesh.shape["emb"]
    in_specs = (P("dp", None, "emb"), P("emb"), P("emb", "head"), P("head"), P("emb", "head"), P("head"), P("emb", None), P(None, "head", None), P(None, "head", None), P(None, "head", None), P("head", None, "emb"))
    out_specs = (P("dp", None, "emb"), P("dp", None, "head"), P("dp", None, None))

    def local_block(hidden, g_in, w_dq, g_q, w_dkv, g_kv, w_kr, w_uq, w_uk, w_uv, w_o):
        nseq, seq, width = hidden.shape
        rd = w_kr.shape[1]
        soft_scale = MSCALE * MSCALE / math.sqrt(w_uq.shape[2])
        wide = hidden.astype(F32)
        ssq = jnp.sum(wide * wide, axis=-1)
        cos_t, sin_t = rope_tables(seq, rd)
        rope = jnp.concatenate([cos_t, sin_t], axis=1)
        gains = jnp.broadcast_to(jnp.concatenate([g_q, g_kv]).astype(F32)[None, :], (8, g_q.shape[0] + g_kv.shape[0]))
        gin = jnp.broadcast_to(g_in.astype(F32)[None, :], (8, width))
        wd = jnp.concatenate([w_dq, w_dkv, w_kr, jnp.zeros((width, 128 - rd), BF16)], axis=1)
        wq, wk, wv, wo = pack_weights(w_uq, w_uk, w_uv, w_o)
        toks = nseq * seq
        out, ckv, kpe = run_kernel(
            hidden.reshape(toks, width), ssq, gin, gains, rope, rope.T, wd, wq, wk, wv, wo,
            soft_scale, nz, w_uq.shape[0], w_uk.shape[0],
        )[:3]
        return out.reshape(hidden.shape), ckv.reshape(nseq, seq, -1), kpe.reshape(nseq, seq, rd)

    return jax.shard_map(local_block, mesh=mesh, in_specs=in_specs, out_specs=out_specs, check_vma=False)
```

```python
import functools
import math
import jax
import jax.numpy as jnp
from jax import lax
from jax.experimental import pallas as pl
from jax.experimental.pallas import tpu as pltpu
from jax.sharding import PartitionSpec as P

ROPE_BASE = 10000.0
NORM_EPS = 1.0e-6
MSCALE = 0.1 * math.log(40.0) + 1.0
LOG2E = math.log2(math.e)
GH = 4
BS = 2
LEAD = 3
RING = 8
NT = (((1,), (1,)), ((), ()))
F32 = jnp.float32
BF16 = jnp.bfloat16


def rope_tables(seq_len, rope_dim):
    half_dim = rope_dim // 2
    inv_freq = ROPE_BASE ** (-2.0 * jnp.arange(half_dim, dtype=F32) / rope_dim)
    angles = jnp.arange(seq_len, dtype=F32)[:, None] * inv_freq[None, :]
    return jnp.cos(angles), jnp.sin(angles)


def kernel(
    dims,
    h_hbm, ssq, g_in, gains, rope, rope_t, wd_hbm, wq_hbm, wk_hbm, wv_hbm, wo_hbm,
    out_hbm, ckv_hbm, kpe_hbm, latz, lath,
    wd, wq, wk, wv, wo, qa, ka, va, qb, kb, vb, scores, probs, ctx, cqn, ckvn, lato, latn,
    hbuf, part, rsr, cz, o1s, own, o2s, fin, hres, o1r, o2r, cko, kpo, ssr, gnr, rall,
    wsem, hsem, ssem, gsem, rs_s, rs_r, ag_s, ag_r, ag_l, y_s, y_r, d_s, d_r, f_s, f_r,
    ld, o1_s, o1_r, o2_s, o2_r, o3_s, o3_r, o3_l, hr, cko_l, kpo_l,
):
    nb, seq, nz, d_model, q_lora, kv_lora, scale = dims
    blk = BS * seq
    piece = blk // nz
    groups = wq.shape[0]
    width = h_hbm.shape[1]
    half = width // 2
    qc, kc = q_lora // 4, kv_lora // 4
    lat = qc + kc
    rd = kpe_hbm.shape[1]
    z = lax.axis_index("emb")
    head = lax.axis_index("head")
    core = head % 2
    partner = head + 1 - 2 * core
    ypeer = (head + 2) % 4
    diag = (partner + 2) % 4
    others = (partner, ypeer, diag)

    def remote(src, dst, ss, rs, **where):
        return pltpu.make_async_remote_copy(
            src_ref=src, dst_ref=dst, send_sem=ss, recv_sem=rs, device_id=where, device_id_type=pl.DeviceIdType.MESH
        )

    def rows(b):
        return pl.ds(pl.multiple_of(b * blk, blk), blk)

    def zt(d):
        return (z + d) % nz

    def ss_copy(d):
        return remote(ssq, ssr.at[d - 1], ssem.at[0, d - 1], ssem.at[1, d - 1], emb=zt(d))

    def gn_copy(r):
        return remote(gains, gnr.at[r], gsem.at[0, r], gsem.at[1, r], head=others[r])

    def h_copy(b):
        return pltpu.make_async_copy(h_hbm.at[rows(b)], hbuf.at[b % 2], hsem.at[b % 2])

    def rs_copy(b, d):
        src = part.at[b % 2, pl.ds(pl.multiple_of(zt(d) * piece, piece), piece)]
        return remote(src, rsr.at[b % RING, d - 1], rs_s.at[b, d - 1], rs_r.at[b, d - 1], emb=zt(d))

    def own_rows(b):
        return pl.ds(pl.multiple_of(b * blk + z * piece, piece), piece)

    def ag_copy(b, d):
        return remote(cz.at[b % 2], latz.at[own_rows(b)], ag_s.at[b, d - 1], ag_r.at[b, d - 1], emb=zt(d))

    def ag_local(b):
        return pltpu.make_async_copy(cz.at[b % 2], latz.at[own_rows(b)], ag_l.at[b % 2])

    def y_copy(b):
        return remote(latz.at[rows(b), pl.ds(0, lat)], lath.at[1, rows(b)], y_s.at[b], y_r.at[b], head=ypeer)

    def d_copy(b):
        return remote(latz.at[rows(b), pl.ds(0, lat)], lath.at[0, rows(b)], d_s.at[b], d_r.at[b], head=partner)

    def f_copy(b):
        return remote(lath.at[1, rows(b)], lath.at[2, rows(b)], f_s.at[b], f_r.at[b], head=partner)

    def loads(b):
        return [pltpu.make_async_copy(latz.at[rows(b)], lato, ld.at[0])] + [
            pltpu.make_async_copy(lath.at[r, rows(b)], latn.at[r], ld.at[1 + r]) for r in range(3)
        ]

    def o1_copy(b):
        return remote(o1s.at[b % 2], o1r.at[b % RING], o1_s.at[b], o1_r.at[b], head=partner)

    def o2_copy(b):
        return remote(o2s.at[b % 2], o2r.at[b % RING], o2_s.at[b], o2_r.at[b], head=ypeer)

    def my_half():
        return pl.ds(pl.multiple_of(core * half, half), half)

    def o3_copy(b):
        return remote(fin.at[b % 2], out_hbm.at[rows(b), my_half()], o3_s.at[b], o3_r.at[b], head=partner)

    def o3_local(b):
        return pltpu.make_async_copy(fin.at[b % 2], out_hbm.at[rows(b), my_half()], o3_l.at[b % 2])

    def hr_copy(b):
        return pltpu.make_async_copy(h_hbm.at[rows(b), my_half()], hres.at[b % 2], hr.at[b % 2])

    def cko_copy(b):
        return pltpu.make_async_copy(cko.at[b % 2], ckv_hbm.at[rows(b)], cko_l.at[b % 2])

    def kpo_copy(b):
        return pltpu.make_async_copy(kpo.at[b % 2], kpe_hbm.at[rows(b)], kpo_l.at[b % 2])

    mine = pl.ds(pl.multiple_of(core * half, half), half)
    theirs = pl.ds(pl.multiple_of((1 - core) * half, half), half)
    weight_copies = [
        pltpu.make_async_copy(wd_hbm, wd, wsem.at[0]),
        pltpu.make_async_copy(wq_hbm, wq, wsem.at[1]),
        pltpu.make_async_copy(wk_hbm, wk, wsem.at[2]),
        pltpu.make_async_copy(wv_hbm, wv, wsem.at[3]),
        pltpu.make_async_copy(wo_hbm.at[mine], wo.at[pl.ds(0, half)], wsem.at[4]),
        pltpu.make_async_copy(wo_hbm.at[theirs], wo.at[pl.ds(half, half)], wsem.at[5]),
    ]
    weight_copies[0].start()
    h_copy(0).start()

    barrier = pltpu.get_barrier_semaphore()
    for d in range(1, nz):
        pl.semaphore_signal(barrier, inc=1, device_id={"emb": zt(d)}, device_id_type=pl.DeviceIdType.MESH)
    for other in others:
        pl.semaphore_signal(barrier, inc=1, device_id={"head": other}, device_id_type=pl.DeviceIdType.MESH)
    pl.semaphore_wait(barrier, nz - 1 + 3)

    for d in range(1, nz):
        ss_copy(d).start()
    for r in range(3):
        gn_copy(r).start()
    for copy in weight_copies[1:]:
        copy.start()
    weight_copies[0].wait()
    total = ssq[...]
    for d in range(1, nz):
        ss_copy(d).wait()
        total = total + ssr[d - 1]
    rall[...] = lax.rsqrt(total / d_model + NORM_EPS)

    def down(b):
        h_copy(b).wait()

        @pl.when(b + 1 < nb)
        def _():
            h_copy(b + 1).start()

        @pl.when(b >= 2)
        def _():
            for d in range(1, nz):
                rs_copy(b - 2, d).wait_send()

        for s in range(BS):
            stat = jnp.transpose(jnp.broadcast_to(rall[pl.ds(b * BS + s, 1), :], (seq, seq)))[:, 0:1]
            x = hbuf[b % 2, s * seq:(s + 1) * seq, :].astype(F32)
            hn = (x * stat * g_in[0:1, :]).astype(BF16)
            part[b % 2, s * seq:(s + 1) * seq, :] = jnp.dot(hn, wd[...], preferred_element_type=F32).astype(BF16)
        for d in range(1, nz):
            rs_copy(b, d).start()

    def reduce_z(b):
        for d in range(1, nz):
            rs_copy(b, d).wait_recv()
        acc = part[b % 2, pl.ds(pl.multiple_of(z * piece, piece), piece), :].astype(F32)
        for d in range(1, nz):
            acc = acc + rsr[b % RING, d - 1].astype(F32)

        @pl.when(b >= 2)
        def _():
            for d in range(1, nz):
                ag_copy(b - 2, d).wait_send()

        cz[b % 2] = acc.astype(BF16)
        for d in range(1, nz):
            ag_copy(b, d).start()
        ag_local(b).start()

    def spread(b):
        for d in range(1, nz):
            ag_copy(b, d).wait_recv()
        ag_local(b).wait()
        y_copy(b).start()
        d_copy(b).start()

    def forward(b):
        y_copy(b).wait_recv()
        f_copy(b).start()

    def fetch(b):
        d_copy(b).wait_recv()
        f_copy(b).wait_recv()
        y_copy(b).wait_send()
        d_copy(b).wait_send()
        f_copy(b).wait_send()
        for copy in loads(b):
            copy.start()

    def normalize(b):
        for copy in loads(b):
            copy.wait()

        @pl.when(b >= 2)
        def _():
            cko_copy(b - 2).wait()
            kpo_copy(b - 2).wait()

        @pl.when(b == 0)
        def _():
            for r in range(3):
                gn_copy(r).wait()

        def latent(r, lo, hi):
            return (lato[:, lo:hi] if r == 0 else latn[r - 1, :, lo:hi]).astype(F32)

        def gain(r, lo, hi):
            return gains[0:1, lo:hi] if r == 0 else gnr[r - 1, 0:1, lo:hi]

        order = (head,) + others
        for lo, hi, full, dst in ((0, qc, q_lora, cqn), (qc, lat, kv_lora, ckvn)):
            sq = None
            for r in range(4):
                x = latent(r, lo, hi)
                one = jnp.sum(x * x, axis=1, keepdims=True)
                sq = one if sq is None else sq + one
            stat = lax.rsqrt(sq / full + NORM_EPS)
            for r in range(4):
                y = (latent(r, lo, hi) * stat * gain(r, lo, hi)).astype(BF16)
                dst[:, pl.ds(pl.multiple_of(order[r] * (hi - lo), 128), hi - lo)] = y
                if r == 0 and lo == qc:
                    cko[b % 2] = y
        for s in range(BS):
            u = lato[s * seq:(s + 1) * seq, lat:lat + rd].astype(F32)
            fr, bk = u[:, :rd // 2], u[:, rd // 2:]
            cos_n, sin_n = rope[:, :rd // 2], rope[:, rd // 2:]
            kpo[b % 2, s * seq:(s + 1) * seq, :] = jnp.concatenate(
                [fr * cos_n - bk * sin_n, fr * sin_n + bk * cos_n], axis=1
            ).astype(BF16)
        cko_copy(b).start()
        kpo_copy(b).start()

    causal = lax.broadcasted_iota(jnp.int32, (seq, seq), 0) <= lax.broadcasted_iota(jnp.int32, (seq, seq), 1)

    def project(g, q, k, v):
        q[...] = lax.dot_general(wq[g], cqn[...], NT, preferred_element_type=F32).astype(BF16)
        k[...] = lax.dot_general(ckvn[...], wk[g], NT, preferred_element_type=F32).astype(BF16)
        v[...] = lax.dot_general(wv[g], ckvn[...], NT, preferred_element_type=F32).astype(BF16)

    def score(b, u, q, k):
        cols, i, hd = slice(u // GH * seq, (u // GH + 1) * seq), u % GH, rd // 2
        cos_t, sin_t = rope_t[0:hd, :], rope_t[hd:rd, :]
        base = i * (128 + rd)
        fr = q[base + 128:base + 128 + hd, cols].astype(F32)
        bk = q[base + 128 + hd:base + 128 + rd, cols].astype(F32)
        q_cat = jnp.concatenate(
            [q[base:base + 128, cols], (fr * cos_t - bk * sin_t).astype(BF16), (fr * sin_t + bk * cos_t).astype(BF16)], axis=0
        )
        k_cat = jnp.concatenate([k[cols, i * 128:(i + 1) * 128], kpo[b % 2, cols, :]], axis=1)
        return jnp.dot(k_cat, q_cat, preferred_element_type=F32)

    def softmax(sc):
        sc = jnp.where(causal, sc, -jnp.inf)
        top = jnp.max(sc, axis=0, keepdims=True)
        e = jnp.exp2((sc - top) * (scale * LOG2E))
        return (e * (1.0 / jnp.sum(e, axis=0, keepdims=True))).astype(BF16)

    def attend(b, g, q, k, v):
        units = range(GH * BS)
        for u in units:
            scores[u] = score(b, u, q, k)
        for u in units:
            probs[u] = softmax(scores[u])
        for u in units:
            cols, i = slice(u // GH * seq, (u // GH + 1) * seq), u % GH
            o = jnp.dot(v[i * 128:(i + 1) * 128, cols], probs[u], preferred_element_type=F32)
            ctx[pl.ds(pl.multiple_of(g * (GH * 128) + i * 128, 128), 128), cols] = o.astype(BF16)

    def begin(b):
        @pl.when(b == 0)
        def _():
            for copy in weight_copies[1:]:
                copy.wait()

        project(0, qa, ka, va)

    def two(b, j):
        g = 2 * j
        project(g + 1, qb, kb, vb)
        attend(b, g, qa, ka, va)
        project(g + 2, qa, ka, va)
        attend(b, g + 1, qb, kb, vb)

    def finish(b):
        project(groups - 1, qb, kb, vb)
        attend(b, groups - 2, qa, ka, va)
        attend(b, groups - 1, qb, kb, vb)
        out_first(b)

    def out_first(b):
        @pl.when(b >= 2)
        def _():
            o1_copy(b - 2).wait_send()

        o1s[b % 2] = jnp.dot(wo[half:, :], ctx[...], preferred_element_type=F32).astype(BF16)
        o1_copy(b).start()
        own[b % 2] = jnp.dot(wo[:half, :], ctx[...], preferred_element_type=F32)

    def out_second(b):
        o1_copy(b).wait_recv()

        @pl.when(b >= 2)
        def _():
            o2_copy(b - 2).wait_send()

        o2s[b % 2] = (own[b % 2] + o1r[b % RING].astype(F32)).astype(BF16)
        o2_copy(b).start()
        hr_copy(b).start()

    def out_third(b):
        o2_copy(b).wait_recv()
        hr_copy(b).wait()

        @pl.when(b >= 2)
        def _():
            o3_copy(b - 2).wait()
            o3_local(b - 2).wait()

        both = o2s[b % 2].astype(F32) + o2r[b % RING].astype(F32)
        fin[b % 2] = (hres[b % 2].astype(F32) + jnp.transpose(both)).astype(BF16)
        o3_copy(b).start()
        o3_local(b).start()

    def step(n, carry):
        i = n - LEAD

        def stage(fn, b):
            pl.when(jnp.logical_and(b >= 0, b < nb))(lambda: fn(b))

        active = jnp.logical_and(i >= 0, i < nb)
        stage(spread, i + 1)
        stage(reduce_z, i + 2)
        stage(down, i + 3)
        stage(normalize, i)
        pl.when(active)(lambda: begin(i))

        def pair(j, c):
            pl.when(active)(lambda: two(i, j))

            @pl.when(j == 0)
            def _():
                stage(forward, i + 1)
                stage(out_third, i - 2)
                stage(out_second, i - 1)

            @pl.when(j == groups // 2 - 2)
            def _():
                stage(fetch, i + 1)

            return c

        lax.fori_loop(0, groups // 2 - 1, pair, 0)
        pl.when(active)(lambda: finish(i))
        return carry

    lax.fori_loop(0, nb + LEAD + 2, step, 0)

    for b in (nb - 2, nb - 1):
        for d in range(1, nz):
            rs_copy(b, d).wait_send()
            ag_copy(b, d).wait_send()
        o1_copy(b).wait_send()
        o2_copy(b).wait_send()
        o3_copy(b).wait()
        o3_local(b).wait()
        cko_copy(b).wait()
        kpo_copy(b).wait()


def run_kernel(h, ssq, g_in, gains, rope, rope_t, wd, wq, wk, wv, wo, scale, nz, q_lora, kv_lora):
    toks, width = h.shape
    seq = rope.shape[0]
    rd = rope.shape[1]
    nb = toks // (BS * seq)
    blk, half = BS * seq, width // 2
    piece = blk // nz
    lat = q_lora // 4 + kv_lora // 4
    latw = wd.shape[1]
    dims = (nb, seq, nz, width * nz, q_lora, kv_lora, scale)
    dma = lambda *s: pltpu.SemaphoreType.DMA(s)
    vm = lambda *s: pltpu.VMEM(s, BF16)
    vf = lambda *s: pltpu.VMEM(s, F32)
    vmem = pl.BlockSpec(memory_space=pltpu.VMEM)
    anyw = pl.BlockSpec(memory_space=pl.ANY)
    gr = GH * 128
    proj = lambda: [vm(wq.shape[1], blk), vm(blk, gr), vm(gr, blk)]
    shape = jax.ShapeDtypeStruct
    scratch = (
        [vm(*wd.shape), vm(*wq.shape), vm(*wk.shape), vm(*wv.shape), vm(*wo.shape)]
        + proj() + proj() + [vf(GH * BS, seq, seq), vm(GH * BS, seq, seq)]
        + [vm(wo.shape[1], blk), vm(blk, q_lora), vm(blk, kv_lora), vm(blk, latw), vm(3, blk, lat)]
        + [vm(2, blk, width), vm(2, blk, latw), vm(RING, nz - 1, piece, latw), vm(2, piece, latw)]
        + [vm(2, half, blk), vf(2, half, blk), vm(2, half, blk), vm(2, blk, half), vm(2, blk, half)]
        + [vm(RING, half, blk), vm(RING, half, blk), vm(2, blk, kv_lora // 4), vm(2, blk, rd)]
        + [vf(nz - 1, *ssq.shape), vf(3, *gains.shape), vf(*ssq.shape)]
        + [dma(6), dma(2), dma(2, nz - 1), dma(2, 3)]
        + [dma(nb, nz - 1)] * 4 + [dma(2)] + [dma(nb)] * 6
        + [dma(4)] + [dma(nb)] * 6 + [dma(2)] * 4
    )
    return pl.pallas_call(
        functools.partial(kernel, dims),
        out_shape=[
            shape((toks, width), BF16), shape((toks, kv_lora // 4), BF16), shape((toks, rd), BF16),
            shape((toks, latw), BF16), shape((3, toks, lat), BF16),
        ],
        in_specs=[anyw] + [vmem] * 5 + [anyw] * 5,
        out_specs=[anyw] * 5,
        scratch_shapes=scratch,
        compiler_params=pltpu.CompilerParams(collective_id=0, has_side_effects=True, vmem_limit_bytes=67_043_328),
        cost_estimate=pl.CostEstimate(flops=171_000_000_000, bytes_accessed=100_000_000, transcendentals=17_000_000),
        name="mla_block",
    )(h, ssq, g_in, gains, rope, rope_t, wd, wq, wk, wv, wo)


def pack_weights(w_uq, w_uk, w_uv, w_o):
    cdim, heads, qk = w_uq.shape
    kdim, _, nope = w_uk.shape
    groups = heads // GH
    wq = w_uq.transpose(1, 2, 0).reshape(groups, GH * qk, cdim)
    wk = w_uk.transpose(1, 2, 0).reshape(groups, GH * nope, kdim)
    wv = w_uv.transpose(1, 2, 0).reshape(groups, GH * w_uv.shape[2], kdim)
    wo = w_o.reshape(heads * w_o.shape[1], w_o.shape[2]).T
    return wq, wk, wv, wo


def solution(mesh):
    nz = mesh.shape["emb"]
    in_specs = (P("dp", None, "emb"), P("emb"), P("emb", "head"), P("head"), P("emb", "head"), P("head"), P("emb", None), P(None, "head", None), P(None, "head", None), P(None, "head", None), P("head", None, "emb"))
    out_specs = (P("dp", None, "emb"), P("dp", None, "head"), P("dp", None, None))

    def local_block(hidden, g_in, w_dq, g_q, w_dkv, g_kv, w_kr, w_uq, w_uk, w_uv, w_o):
        nseq, seq, width = hidden.shape
        rd = w_kr.shape[1]
        soft_scale = MSCALE * MSCALE / math.sqrt(w_uq.shape[2])
        wide = hidden.astype(F32)
        ssq = jnp.sum(wide * wide, axis=-1)
        cos_t, sin_t = rope_tables(seq, rd)
        rope = jnp.concatenate([cos_t, sin_t], axis=1)
        gains = jnp.broadcast_to(jnp.concatenate([g_q, g_kv]).astype(F32)[None, :], (8, g_q.shape[0] + g_kv.shape[0]))
        gin = jnp.broadcast_to(g_in.astype(F32)[None, :], (8, width))
        wd = jnp.concatenate([w_dq, w_dkv, w_kr, jnp.zeros((width, 128 - rd), BF16)], axis=1)
        wq, wk, wv, wo = pack_weights(w_uq, w_uk, w_uv, w_o)
        toks = nseq * seq
        out, ckv, kpe = run_kernel(
            hidden.reshape(toks, width), ssq, gin, gains, rope, rope.T, wd, wq, wk, wv, wo,
            soft_scale, nz, w_uq.shape[0], w_uk.shape[0],
        )[:3]
        return out.reshape(hidden.shape), ckv.reshape(nseq, seq, -1), kpe.reshape(nseq, seq, rd)

    return jax.shard_map(local_block, mesh=mesh, in_specs=in_specs, out_specs=out_specs, check_vma=False)
```

```python
import functools
import math
import jax
import jax.numpy as jnp
from jax import lax
from jax.experimental import pallas as pl
from jax.experimental.pallas import tpu as pltpu
from jax.sharding import PartitionSpec as P

ROPE_BASE = 10000.0
NORM_EPS = 1.0e-6
MSCALE = 0.1 * math.log(40.0) + 1.0
LOG2E = math.log2(math.e)
GH = 4
BS = 2
LEAD = 3
RING = 8
NT = (((1,), (1,)), ((), ()))
F32 = jnp.float32
BF16 = jnp.bfloat16


def rope_tables(seq_len, rope_dim):
    half_dim = rope_dim // 2
    inv_freq = ROPE_BASE ** (-2.0 * jnp.arange(half_dim, dtype=F32) / rope_dim)
    angles = jnp.arange(seq_len, dtype=F32)[:, None] * inv_freq[None, :]
    return jnp.cos(angles), jnp.sin(angles)


def kernel(
    dims,
    h_hbm, ssq, g_in, gains, rope, rope_t, wd_hbm, wq_hbm, wk_hbm, wv_hbm, wo_hbm,
    out_hbm, ckv_hbm, kpe_hbm, latz, lath,
    wd, wq, wk, wv, wo, qa, ka, va, qb, kb, vb, scores, probs, ctx, cqn, ckvn, lato, latn,
    hbuf, part, rsr, cz, o1s, own, o2s, fin, hres, o1r, o2r, cko, kpo, ssr, gnr, rall,
    wsem, hsem, ssem, gsem, rs_s, rs_r, ag_s, ag_r, ag_l, y_s, y_r, d_s, d_r, f_s, f_r,
    ld, o1_s, o1_r, o2_s, o2_r, o3_s, o3_r, o3_l, hr, cko_l, kpo_l,
):
    nb, seq, nz, d_model, q_lora, kv_lora, scale = dims
    blk = BS * seq
    piece = blk // nz
    groups = wq.shape[0]
    width = h_hbm.shape[1]
    half = width // 2
    qc, kc = q_lora // 4, kv_lora // 4
    lat = qc + kc
    rd = kpe_hbm.shape[1]
    z = lax.axis_index("emb")
    head = lax.axis_index("head")
    core = head % 2
    partner = head + 1 - 2 * core
    ypeer = (head + 2) % 4
    diag = (partner + 2) % 4
    others = (partner, ypeer, diag)

    def remote(src, dst, ss, rs, **where):
        return pltpu.make_async_remote_copy(
            src_ref=src, dst_ref=dst, send_sem=ss, recv_sem=rs, device_id=where, device_id_type=pl.DeviceIdType.MESH
        )

    def rows(b):
        return pl.ds(pl.multiple_of(b * blk, blk), blk)

    def zt(d):
        return (z + d) % nz

    def ss_copy(d):
        return remote(ssq, ssr.at[d - 1], ssem.at[0, d - 1], ssem.at[1, d - 1], emb=zt(d))

    def gn_copy(r):
        return remote(gains, gnr.at[r], gsem.at[0, r], gsem.at[1, r], head=others[r])

    def h_copy(b):
        return pltpu.make_async_copy(h_hbm.at[rows(b)], hbuf.at[b % 2], hsem.at[b % 2])

    def rs_copy(b, d):
        src = part.at[b % 2, pl.ds(pl.multiple_of(zt(d) * piece, piece), piece)]
        return remote(src, rsr.at[b % RING, d - 1], rs_s.at[b, d - 1], rs_r.at[b, d - 1], emb=zt(d))

    def own_rows(b):
        return pl.ds(pl.multiple_of(b * blk + z * piece, piece), piece)

    def ag_copy(b, d):
        return remote(cz.at[b % 2], latz.at[own_rows(b)], ag_s.at[b, d - 1], ag_r.at[b, d - 1], emb=zt(d))

    def ag_local(b):
        return pltpu.make_async_copy(cz.at[b % 2], latz.at[own_rows(b)], ag_l.at[b % 2])

    def y_copy(b):
        return remote(latz.at[rows(b), pl.ds(0, lat)], lath.at[1, rows(b)], y_s.at[b], y_r.at[b], head=ypeer)

    def d_copy(b):
        return remote(latz.at[rows(b), pl.ds(0, lat)], lath.at[0, rows(b)], d_s.at[b], d_r.at[b], head=partner)

    def f_copy(b):
        return remote(lath.at[1, rows(b)], lath.at[2, rows(b)], f_s.at[b], f_r.at[b], head=partner)

    def loads(b):
        return [pltpu.make_async_copy(latz.at[rows(b)], lato, ld.at[0])] + [
            pltpu.make_async_copy(lath.at[r, rows(b)], latn.at[r], ld.at[1 + r]) for r in range(3)
        ]

    def o1_copy(b):
        return remote(o1s.at[b % 2], o1r.at[b % RING], o1_s.at[b], o1_r.at[b], head=partner)

    def o2_copy(b):
        return remote(o2s.at[b % 2], o2r.at[b % RING], o2_s.at[b], o2_r.at[b], head=ypeer)

    def my_half():
        return pl.ds(pl.multiple_of(core * half, half), half)

    def o3_copy(b):
        return remote(fin.at[b % 2], out_hbm.at[rows(b), my_half()], o3_s.at[b], o3_r.at[b], head=partner)

    def o3_local(b):
        return pltpu.make_async_copy(fin.at[b % 2], out_hbm.at[rows(b), my_half()], o3_l.at[b % 2])

    def hr_copy(b):
        return pltpu.make_async_copy(h_hbm.at[rows(b), my_half()], hres.at[b % 2], hr.at[b % 2])

    def cko_copy(b):
        return pltpu.make_async_copy(cko.at[b % 2], ckv_hbm.at[rows(b)], cko_l.at[b % 2])

    def kpo_copy(b):
        return pltpu.make_async_copy(kpo.at[b % 2], kpe_hbm.at[rows(b)], kpo_l.at[b % 2])

    weight_copies = [
        pltpu.make_async_copy(wd_hbm, wd, wsem.at[0]),
        pltpu.make_async_copy(wq_hbm, wq, wsem.at[1]),
        pltpu.make_async_copy(wk_hbm, wk, wsem.at[2]),
        pltpu.make_async_copy(wv_hbm, wv, wsem.at[3]),
    ]

    def wo_chunk(j):
        at = pl.ds(pl.multiple_of((core * half + j * 128) % width, 128), 128)
        return pltpu.make_async_copy(wo_hbm.at[:, at], ctx.at[:, pl.ds(j % 2 * 128, 128)], wsem.at[4 + j % 2])

    def turn(j):
        wo_chunk(j).wait()
        wo[j * 128:(j + 1) * 128, :] = jnp.transpose(ctx[:, j % 2 * 128:(j % 2 + 1) * 128].astype(F32)).astype(BF16)
        if (j + 2) * 128 < width:
            wo_chunk(j + 2).start()

    weight_copies[0].start()
    h_copy(0).start()
    wo_chunk(0).start()
    wo_chunk(1).start()

    barrier = pltpu.get_barrier_semaphore()
    for d in range(1, nz):
        pl.semaphore_signal(barrier, inc=1, device_id={"emb": zt(d)}, device_id_type=pl.DeviceIdType.MESH)
    for other in others:
        pl.semaphore_signal(barrier, inc=1, device_id={"head": other}, device_id_type=pl.DeviceIdType.MESH)
    pl.semaphore_wait(barrier, nz - 1 + 3)

    for d in range(1, nz):
        ss_copy(d).start()
    for r in range(3):
        gn_copy(r).start()
    for copy in weight_copies[1:]:
        copy.start()
    weight_copies[0].wait()
    total = ssq[...]
    for d in range(1, nz):
        ss_copy(d).wait()
        total = total + ssr[d - 1]
    rall[...] = lax.rsqrt(total / d_model + NORM_EPS)

    def down(b):
        h_copy(b).wait()

        @pl.when(b + 1 < nb)
        def _():
            h_copy(b + 1).start()

        @pl.when(b >= 2)
        def _():
            for d in range(1, nz):
                rs_copy(b - 2, d).wait_send()

        hn = []
        for s in range(BS):
            stat = jnp.transpose(jnp.broadcast_to(rall[pl.ds(b * BS + s, 1), :], (seq, seq)))[:, 0:1]
            x = hbuf[b % 2, s * seq:(s + 1) * seq, :].astype(F32)
            hn.append((x * stat * g_in[0:1, :]).astype(BF16))
        part[b % 2] = jnp.dot(jnp.concatenate(hn, axis=0), wd[...], preferred_element_type=F32).astype(BF16)
        for d in range(1, nz):
            rs_copy(b, d).start()

    def reduce_z(b):
        for d in range(1, nz):
            rs_copy(b, d).wait_recv()
        acc = part[b % 2, pl.ds(pl.multiple_of(z * piece, piece), piece), :].astype(F32)
        for d in range(1, nz):
            acc = acc + rsr[b % RING, d - 1].astype(F32)

        @pl.when(b >= 2)
        def _():
            for d in range(1, nz):
                ag_copy(b - 2, d).wait_send()

        cz[b % 2] = acc.astype(BF16)
        for d in range(1, nz):
            ag_copy(b, d).start()
        ag_local(b).start()

    def spread(b):
        for d in range(1, nz):
            ag_copy(b, d).wait_recv()
        ag_local(b).wait()
        y_copy(b).start()
        d_copy(b).start()

    def forward(b):
        y_copy(b).wait_recv()
        f_copy(b).start()

    def fetch(b):
        d_copy(b).wait_recv()
        f_copy(b).wait_recv()
        y_copy(b).wait_send()
        d_copy(b).wait_send()
        f_copy(b).wait_send()
        for copy in loads(b):
            copy.start()

    front = lax.broadcasted_iota(jnp.int32, (seq, 128), 1) < rd // 2

    def normalize(b):
        for copy in loads(b):
            copy.wait()

        @pl.when(b >= 2)
        def _():
            cko_copy(b - 2).wait()
            kpo_copy(b - 2).wait()

        @pl.when(b == 0)
        def _():
            for r in range(3):
                gn_copy(r).wait()

        def latent(r, lo, hi):
            return (lato[:, lo:hi] if r == 0 else latn[r - 1, :, lo:hi]).astype(F32)

        def gain(r, lo, hi):
            return gains[0:1, lo:hi] if r == 0 else gnr[r - 1, 0:1, lo:hi]

        order = (head,) + others
        for lo, hi, full, dst in ((0, qc, q_lora, cqn), (qc, lat, kv_lora, ckvn)):
            acc = None
            for r in range(4):
                for t in range(lo, hi, 128):
                    x = latent(r, t, t + 128)
                    acc = x * x if acc is None else acc + x * x
            sq = jnp.sum(acc, axis=1, keepdims=True)
            stat = lax.rsqrt(sq / full + NORM_EPS)
            for r in range(4):
                y = (latent(r, lo, hi) * stat * gain(r, lo, hi)).astype(BF16)
                dst[:, pl.ds(pl.multiple_of(order[r] * (hi - lo), 128), hi - lo)] = y
                if r == 0 and lo == qc:
                    cko[b % 2] = y
        for s in range(BS):
            u = lato[s * seq:(s + 1) * seq, lat:lat + 128].astype(F32)
            swapped = jnp.where(front, pltpu.roll(u, 128 - rd // 2, 1), pltpu.roll(u, rd // 2, 1))
            turned = u * rope[:, 0:128] + swapped * rope[:, 128:256]
            kpo[b % 2, s * seq:(s + 1) * seq, :] = turned[:, :rd].astype(BF16)
        cko_copy(b).start()
        kpo_copy(b).start()

    causal = lax.broadcasted_iota(jnp.int32, (seq, seq), 0) <= lax.broadcasted_iota(jnp.int32, (seq, seq), 1)

    def project(g, q, k, v):
        q[...] = lax.dot_general(wq[g], cqn[...], NT, preferred_element_type=F32).astype(BF16)
        k[...] = lax.dot_general(ckvn[...], wk[g], NT, preferred_element_type=F32).astype(BF16)
        v[...] = lax.dot_general(wv[g], ckvn[...], NT, preferred_element_type=F32).astype(BF16)

    def score(b, u, q, k):
        cols, i, hd = slice(u // GH * seq, (u // GH + 1) * seq), u % GH, rd // 2
        cos_t, sin_t = rope_t[0:hd, :], rope_t[hd:rd, :]
        base = i * (128 + rd)
        fr = q[base + 128:base + 128 + hd, cols].astype(F32)
        bk = q[base + 128 + hd:base + 128 + rd, cols].astype(F32)
        q_cat = jnp.concatenate(
            [q[base:base + 128, cols], (fr * cos_t - bk * sin_t).astype(BF16), (fr * sin_t + bk * cos_t).astype(BF16)], axis=0
        )
        k_cat = jnp.concatenate([k[cols, i * 128:(i + 1) * 128], kpo[b % 2, cols, :]], axis=1)
        return jnp.dot(k_cat, q_cat, preferred_element_type=F32)

    def softmax(sc):
        sc = jnp.where(causal, sc, -jnp.inf)
        top = jnp.max(sc, axis=0, keepdims=True)
        e = jnp.exp2((sc - top) * (scale * LOG2E))
        return (e * (1.0 / jnp.sum(e, axis=0, keepdims=True))).astype(BF16)

    def attend(b, g, q, k, v):
        units = range(GH * BS)
        for u in units:
            scores[u] = score(b, u, q, k)
        for u in units:
            probs[u] = softmax(scores[u])
        for u in units:
            cols, i = slice(u // GH * seq, (u // GH + 1) * seq), u % GH
            o = jnp.dot(v[i * 128:(i + 1) * 128, cols], probs[u], preferred_element_type=F32)
            ctx[pl.ds(pl.multiple_of(g * (GH * 128) + i * 128, 128), 128), cols] = o.astype(BF16)

    def begin(b):
        @pl.when(b == 0)
        def _():
            for copy in weight_copies[1:]:
                copy.wait()

        project(0, qa, ka, va)

    def two(b, j):
        g = 2 * j
        project(g + 1, qb, kb, vb)
        attend(b, g, qa, ka, va)
        project(g + 2, qa, ka, va)
        attend(b, g + 1, qb, kb, vb)

    def finish(b):
        project(groups - 1, qb, kb, vb)
        attend(b, groups - 2, qa, ka, va)
        attend(b, groups - 1, qb, kb, vb)
        out_first(b)

    def out_first(b):
        @pl.when(b >= 2)
        def _():
            o1_copy(b - 2).wait_send()

        o1s[b % 2] = jnp.dot(wo[half:, :], ctx[...], preferred_element_type=F32).astype(BF16)
        o1_copy(b).start()
        own[b % 2] = jnp.dot(wo[:half, :], ctx[...], preferred_element_type=F32)

    def out_second(b):
        o1_copy(b).wait_recv()

        @pl.when(b >= 2)
        def _():
            o2_copy(b - 2).wait_send()

        o2s[b % 2] = (own[b % 2] + o1r[b % RING].astype(F32)).astype(BF16)
        o2_copy(b).start()
        hr_copy(b).start()

    def out_third(b):
        o2_copy(b).wait_recv()
        hr_copy(b).wait()

        @pl.when(b >= 2)
        def _():
            o3_copy(b - 2).wait()
            o3_local(b - 2).wait()

        both = o2s[b % 2].astype(F32) + o2r[b % RING].astype(F32)
        fin[b % 2] = (hres[b % 2].astype(F32) + jnp.transpose(both)).astype(BF16)
        o3_copy(b).start()
        o3_local(b).start()

    def step(n, carry):
        i = n - LEAD

        def stage(fn, b):
            pl.when(jnp.logical_and(b >= 0, b < nb))(lambda: fn(b))

        active = jnp.logical_and(i >= 0, i < nb)
        stage(reduce_z, i + 2)
        stage(down, i + 3)
        chunks = width // 128
        for m in range(LEAD):
            @pl.when(n == m)
            def _():
                for j in range(chunks * m // LEAD, chunks * (m + 1) // LEAD):
                    turn(j)

        stage(normalize, i)
        pl.when(active)(lambda: begin(i))

        def pair(j, c):
            pl.when(active)(lambda: two(i, j))

            @pl.when(j == 0)
            def _():
                stage(forward, i + 1)
                stage(out_third, i - 2)
                stage(out_second, i - 1)

            @pl.when(j == groups // 2 - 2)
            def _():
                stage(fetch, i + 1)
                stage(spread, i + 2)

            return c

        lax.fori_loop(0, groups // 2 - 1, pair, 0)
        pl.when(active)(lambda: finish(i))
        return carry

    lax.fori_loop(0, nb + LEAD + 2, step, 0)

    for b in (nb - 2, nb - 1):
        for d in range(1, nz):
            rs_copy(b, d).wait_send()
            ag_copy(b, d).wait_send()
        o1_copy(b).wait_send()
        o2_copy(b).wait_send()
        o3_copy(b).wait()
        o3_local(b).wait()
        cko_copy(b).wait()
        kpo_copy(b).wait()


def run_kernel(h, ssq, g_in, gains, rope, rope_t, wd, wq, wk, wv, wo, scale, nz, q_lora, kv_lora):
    toks, width = h.shape
    seq, rd = rope.shape[0], rope_t.shape[0]
    nb = toks // (BS * seq)
    blk, half = BS * seq, width // 2
    piece = blk // nz
    lat = q_lora // 4 + kv_lora // 4
    latw = wd.shape[1]
    dims = (nb, seq, nz, width * nz, q_lora, kv_lora, scale)
    dma = lambda *s: pltpu.SemaphoreType.DMA(s)
    vm = lambda *s: pltpu.VMEM(s, BF16)
    vf = lambda *s: pltpu.VMEM(s, F32)
    vmem = pl.BlockSpec(memory_space=pltpu.VMEM)
    anyw = pl.BlockSpec(memory_space=pl.ANY)
    gr = GH * 128
    proj = lambda: [vm(wq.shape[1], blk), vm(blk, gr), vm(gr, blk)]
    shape = jax.ShapeDtypeStruct
    scratch = (
        [vm(*wd.shape), vm(*wq.shape), vm(*wk.shape), vm(*wv.shape), vm(*wo.shape[::-1])]
        + proj() + proj() + [vf(GH * BS, seq, seq), vm(GH * BS, seq, seq)]
        + [vm(wo.shape[0], blk), vm(blk, q_lora), vm(blk, kv_lora), vm(blk, latw), vm(3, blk, lat)]
        + [vm(2, blk, width), vm(2, blk, latw), vm(RING, nz - 1, piece, latw), vm(2, piece, latw)]
        + [vm(2, half, blk), vf(2, half, blk), vm(2, half, blk), vm(2, blk, half), vm(2, blk, half)]
        + [vm(RING, half, blk), vm(RING, half, blk), vm(2, blk, kv_lora // 4), vm(2, blk, rd)]
        + [vf(nz - 1, *ssq.shape), vf(3, *gains.shape), vf(*ssq.shape)]
        + [dma(6), dma(2), dma(2, nz - 1), dma(2, 3)]
        + [dma(nb, nz - 1)] * 4 + [dma(2)] + [dma(nb)] * 6
        + [dma(4)] + [dma(nb)] * 6 + [dma(2)] * 4
    )
    return pl.pallas_call(
        functools.partial(kernel, dims),
        out_shape=[
            shape((toks, width), BF16), shape((toks, kv_lora // 4), BF16), shape((toks, rd), BF16),
            shape((toks, latw), BF16), shape((3, toks, lat), BF16),
        ],
        in_specs=[anyw] + [vmem] * 5 + [anyw] * 5,
        out_specs=[anyw] * 5,
        scratch_shapes=scratch,
        compiler_params=pltpu.CompilerParams(collective_id=0, has_side_effects=True, vmem_limit_bytes=67_043_328),
        cost_estimate=pl.CostEstimate(flops=171_000_000_000, bytes_accessed=100_000_000, transcendentals=17_000_000),
        name="mla_block",
    )(h, ssq, g_in, gains, rope, rope_t, wd, wq, wk, wv, wo)


def pack_weights(w_uq, w_uk, w_uv, w_o):
    cdim, heads, qk = w_uq.shape
    kdim, _, nope = w_uk.shape
    groups = heads // GH
    wq = w_uq.transpose(1, 2, 0).reshape(groups, GH * qk, cdim)
    wk = w_uk.transpose(1, 2, 0).reshape(groups, GH * nope, kdim)
    wv = w_uv.transpose(1, 2, 0).reshape(groups, GH * w_uv.shape[2], kdim)
    wo = w_o.reshape(heads * w_o.shape[1], w_o.shape[2])
    return wq, wk, wv, wo


def solution(mesh):
    nz = mesh.shape["emb"]
    in_specs = (P("dp", None, "emb"), P("emb"), P("emb", "head"), P("head"), P("emb", "head"), P("head"), P("emb", None), P(None, "head", None), P(None, "head", None), P(None, "head", None), P("head", None, "emb"))
    out_specs = (P("dp", None, "emb"), P("dp", None, "head"), P("dp", None, None))

    def local_block(hidden, g_in, w_dq, g_q, w_dkv, g_kv, w_kr, w_uq, w_uk, w_uv, w_o):
        nseq, seq, width = hidden.shape
        rd = w_kr.shape[1]
        soft_scale = MSCALE * MSCALE / math.sqrt(w_uq.shape[2])
        wide = hidden.astype(F32)
        ssq = jnp.sum(wide * wide, axis=-1)
        cos_t, sin_t = rope_tables(seq, rd)
        pad = jnp.zeros((seq, 128 - rd), F32)
        rope = jnp.concatenate([cos_t, cos_t, pad, -sin_t, sin_t, pad], axis=1)
        rope_t = jnp.concatenate([cos_t, sin_t], axis=1).T
        gains = jnp.broadcast_to(jnp.concatenate([g_q, g_kv]).astype(F32)[None, :], (8, g_q.shape[0] + g_kv.shape[0]))
        gin = jnp.broadcast_to(g_in.astype(F32)[None, :], (8, width))
        wd = jnp.concatenate([w_dq, w_dkv, w_kr, jnp.zeros((width, 128 - rd), BF16)], axis=1)
        wq, wk, wv, wo = pack_weights(w_uq, w_uk, w_uv, w_o)
        toks = nseq * seq
        out, ckv, kpe = run_kernel(
            hidden.reshape(toks, width), ssq, gin, gains, rope, rope_t, wd, wq, wk, wv, wo,
            soft_scale, nz, w_uq.shape[0], w_uk.shape[0],
        )[:3]
        return out.reshape(hidden.shape), ckv.reshape(nseq, seq, -1), kpe.reshape(nseq, seq, rd)

    return jax.shard_map(local_block, mesh=mesh, in_specs=in_specs, out_specs=out_specs, check_vma=False)
```

```python
import functools
import math
import jax
import jax.numpy as jnp
from jax import lax
from jax.experimental import pallas as pl
from jax.experimental.pallas import tpu as pltpu
from jax.sharding import PartitionSpec as P

ROPE_BASE = 10000.0
NORM_EPS = 1.0e-6
MSCALE = 0.1 * math.log(40.0) + 1.0
LOG2E = math.log2(math.e)
GH = 4
BS = 2
LEAD = 3
RING = 8
NT = (((1,), (1,)), ((), ()))
F32 = jnp.float32
BF16 = jnp.bfloat16


def rope_tables(seq_len, rope_dim):
    half_dim = rope_dim // 2
    inv_freq = ROPE_BASE ** (-2.0 * jnp.arange(half_dim, dtype=F32) / rope_dim)
    angles = jnp.arange(seq_len, dtype=F32)[:, None] * inv_freq[None, :]
    return jnp.cos(angles), jnp.sin(angles)


def kernel(
    dims,
    h_hbm, ssq, g_in, gains, rope, rope_t, wd_hbm, wq_hbm, wk_hbm, wv_hbm, wo_hbm,
    out_hbm, ckv_hbm, kpe_hbm, latz, lath,
    wd, wq, wk, wv, wo, qa, ka, va, qb, kb, vb, scores, probs, ctx, cqn, ckvn, lato, latn,
    hbuf, part, rsr, cz, o1s, own, o2s, fin, hres, o1r, o2r, cko, kpo, ssr, gnr, rall,
    wsem, hsem, ssem, gsem, rs_s, rs_r, ag_s, ag_r, ag_l, y_s, y_r, d_s, d_r, f_s, f_r,
    ld, o1_s, o1_r, o2_s, o2_r, o3_s, o3_r, o3_l, hr, cko_l, kpo_l,
):
    nb, seq, nz, d_model, q_lora, kv_lora, scale = dims
    blk = BS * seq
    piece = blk // nz
    groups = wq.shape[0]
    width = h_hbm.shape[1]
    half = width // 2
    qc, kc = q_lora // 4, kv_lora // 4
    lat = qc + kc
    rd = kpe_hbm.shape[1]
    z = lax.axis_index("emb")
    head = lax.axis_index("head")
    core = head % 2
    partner = head + 1 - 2 * core
    ypeer = (head + 2) % 4
    diag = (partner + 2) % 4
    others = (partner, ypeer, diag)

    def remote(src, dst, ss, rs, **where):
        return pltpu.make_async_remote_copy(
            src_ref=src, dst_ref=dst, send_sem=ss, recv_sem=rs, device_id=where, device_id_type=pl.DeviceIdType.MESH
        )

    def rows(b):
        return pl.ds(pl.multiple_of(b * blk, blk), blk)

    def zt(d):
        return (z + d) % nz

    def ss_copy(d):
        return remote(ssq, ssr.at[d - 1], ssem.at[0, d - 1], ssem.at[1, d - 1], emb=zt(d))

    def gn_copy(r):
        return remote(gains, gnr.at[r], gsem.at[0, r], gsem.at[1, r], head=others[r])

    def h_copy(b):
        return pltpu.make_async_copy(h_hbm.at[rows(b)], hbuf.at[b % 2], hsem.at[b % 2])

    def rs_copy(b, d):
        src = part.at[b % 2, pl.ds(pl.multiple_of(zt(d) * piece, piece), piece)]
        return remote(src, rsr.at[b % RING, d - 1], rs_s.at[b, d - 1], rs_r.at[b, d - 1], emb=zt(d))

    def own_rows(b):
        return pl.ds(pl.multiple_of(b * blk + z * piece, piece), piece)

    def ag_copy(b, d):
        return remote(cz.at[b % 2], latz.at[own_rows(b)], ag_s.at[b, d - 1], ag_r.at[b, d - 1], emb=zt(d))

    def ag_local(b):
        return pltpu.make_async_copy(cz.at[b % 2], latz.at[own_rows(b)], ag_l.at[b % 2])

    def y_copy(b):
        return remote(latz.at[rows(b), pl.ds(0, lat)], lath.at[1, rows(b)], y_s.at[b], y_r.at[b], head=ypeer)

    def d_copy(b):
        return remote(latz.at[rows(b), pl.ds(0, lat)], lath.at[0, rows(b)], d_s.at[b], d_r.at[b], head=partner)

    def f_copy(b):
        return remote(lath.at[1, rows(b)], lath.at[2, rows(b)], f_s.at[b], f_r.at[b], head=partner)

    def loads(b):
        return [pltpu.make_async_copy(latz.at[rows(b)], lato, ld.at[0])] + [
            pltpu.make_async_copy(lath.at[r, rows(b)], latn.at[r], ld.at[1 + r]) for r in range(3)
        ]

    def o1_copy(b):
        return remote(o1s.at[b % 2], o1r.at[b % RING], o1_s.at[b], o1_r.at[b], head=partner)

    def o2_copy(b):
        return remote(o2s.at[b % 2], o2r.at[b % RING], o2_s.at[b], o2_r.at[b], head=ypeer)

    def my_half():
        return pl.ds(pl.multiple_of(core * half, half), half)

    def o3_copy(b):
        return remote(fin.at[b % 2], out_hbm.at[rows(b), my_half()], o3_s.at[b], o3_r.at[b], head=partner)

    def o3_local(b):
        return pltpu.make_async_copy(fin.at[b % 2], out_hbm.at[rows(b), my_half()], o3_l.at[b % 2])

    def hr_copy(b):
        return pltpu.make_async_copy(h_hbm.at[rows(b), my_half()], hres.at[b % 2], hr.at[b % 2])

    def cko_copy(b):
        return pltpu.make_async_copy(cko.at[b % 2], ckv_hbm.at[rows(b)], cko_l.at[b % 2])

    def kpo_copy(b):
        return pltpu.make_async_copy(kpo.at[b % 2], kpe_hbm.at[rows(b)], kpo_l.at[b % 2])

    weight_copies = [
        pltpu.make_async_copy(wd_hbm, wd, wsem.at[0]),
        pltpu.make_async_copy(wq_hbm, wq, wsem.at[1]),
        pltpu.make_async_copy(wk_hbm, wk, wsem.at[2]),
        pltpu.make_async_copy(wv_hbm, wv, wsem.at[3]),
    ]

    def wo_chunk(j):
        at = pl.ds(pl.multiple_of((core * half + j * 128) % width, 128), 128)
        return pltpu.make_async_copy(wo_hbm.at[:, at], ctx.at[:, pl.ds(j % 2 * 128, 128)], wsem.at[4 + j % 2])

    def turn(j):
        wo_chunk(j).wait()
        wo[j * 128:(j + 1) * 128, :] = jnp.transpose(ctx[:, j % 2 * 128:(j % 2 + 1) * 128].astype(F32)).astype(BF16)
        if (j + 2) * 128 < width:
            wo_chunk(j + 2).start()

    weight_copies[0].start()
    h_copy(0).start()
    wo_chunk(0).start()
    wo_chunk(1).start()

    barrier = pltpu.get_barrier_semaphore()
    for d in range(1, nz):
        pl.semaphore_signal(barrier, inc=1, device_id={"emb": zt(d)}, device_id_type=pl.DeviceIdType.MESH)
    for other in others:
        pl.semaphore_signal(barrier, inc=1, device_id={"head": other}, device_id_type=pl.DeviceIdType.MESH)
    pl.semaphore_wait(barrier, nz - 1 + 3)

    for d in range(1, nz):
        ss_copy(d).start()
    for r in range(3):
        gn_copy(r).start()
    for copy in weight_copies[1:]:
        copy.start()
    weight_copies[0].wait()
    total = ssq[...]
    for d in range(1, nz):
        ss_copy(d).wait()
        total = total + ssr[d - 1]
    rall[...] = lax.rsqrt(total / d_model + NORM_EPS)

    def down(b):
        h_copy(b).wait()

        @pl.when(b + 1 < nb)
        def _():
            h_copy(b + 1).start()

        @pl.when(b >= 2)
        def _():
            for d in range(1, nz):
                rs_copy(b - 2, d).wait_send()

        hn = []
        for s in range(BS):
            stat = jnp.transpose(jnp.broadcast_to(rall[pl.ds(b * BS + s, 1), :], (seq, seq)))[:, 0:1]
            x = hbuf[b % 2, s * seq:(s + 1) * seq, :].astype(F32)
            hn.append((x * stat * g_in[0:1, :]).astype(BF16))
        part[b % 2] = jnp.dot(jnp.concatenate(hn, axis=0), wd[...], preferred_element_type=F32).astype(BF16)
        for d in range(1, nz):
            rs_copy(b, d).start()

    def reduce_z(b):
        for d in range(1, nz):
            rs_copy(b, d).wait_recv()
        acc = part[b % 2, pl.ds(pl.multiple_of(z * piece, piece), piece), :].astype(F32)
        for d in range(1, nz):
            acc = acc + rsr[b % RING, d - 1].astype(F32)

        @pl.when(b >= 2)
        def _():
            for d in range(1, nz):
                ag_copy(b - 2, d).wait_send()

        cz[b % 2] = acc.astype(BF16)
        for d in range(1, nz):
            ag_copy(b, d).start()
        ag_local(b).start()

    def spread(b):
        for d in range(1, nz):
            ag_copy(b, d).wait_recv()
        ag_local(b).wait()
        y_copy(b).start()
        d_copy(b).start()

    def forward(b):
        y_copy(b).wait_recv()
        f_copy(b).start()

    def fetch(b):
        d_copy(b).wait_recv()
        f_copy(b).wait_recv()
        y_copy(b).wait_send()
        d_copy(b).wait_send()
        f_copy(b).wait_send()
        for copy in loads(b):
            copy.start()

    front = lax.broadcasted_iota(jnp.int32, (seq, 128), 1) < rd // 2

    def normalize(b):
        for copy in loads(b):
            copy.wait()

        @pl.when(b >= 2)
        def _():
            cko_copy(b - 2).wait()
            kpo_copy(b - 2).wait()

        @pl.when(b == 0)
        def _():
            for r in range(3):
                gn_copy(r).wait()

        def latent(r, lo, hi):
            return (lato[:, lo:hi] if r == 0 else latn[r - 1, :, lo:hi]).astype(F32)

        def gain(r, lo, hi):
            return gains[0:1, lo:hi] if r == 0 else gnr[r - 1, 0:1, lo:hi]

        order = (head,) + others
        for lo, hi, full, dst in ((0, qc, q_lora, cqn), (qc, lat, kv_lora, ckvn)):
            acc = None
            for r in range(4):
                for t in range(lo, hi, 128):
                    x = latent(r, t, t + 128)
                    acc = x * x if acc is None else acc + x * x
            sq = jnp.sum(acc, axis=1, keepdims=True)
            stat = lax.rsqrt(sq / full + NORM_EPS)
            for r in range(4):
                y = (latent(r, lo, hi) * stat * gain(r, lo, hi)).astype(BF16)
                dst[:, pl.ds(pl.multiple_of(order[r] * (hi - lo), 128), hi - lo)] = y
                if r == 0 and lo == qc:
                    cko[b % 2] = y
        for s in range(BS):
            u = lato[s * seq:(s + 1) * seq, lat:lat + 128].astype(F32)
            swapped = jnp.where(front, pltpu.roll(u, 128 - rd // 2, 1), pltpu.roll(u, rd // 2, 1))
            turned = u * rope[:, 0:128] + swapped * rope[:, 128:256]
            kpo[b % 2, s * seq:(s + 1) * seq, :] = turned[:, :rd].astype(BF16)
        cko_copy(b).start()
        kpo_copy(b).start()

    causal = lax.broadcasted_iota(jnp.int32, (seq, seq), 0) <= lax.broadcasted_iota(jnp.int32, (seq, seq), 1)

    def project(g, q, k, v):
        q[...] = lax.dot_general(wq[g], cqn[...], NT, preferred_element_type=F32).astype(BF16)
        k[...] = lax.dot_general(ckvn[...], wk[g], NT, preferred_element_type=F32).astype(BF16)
        v[...] = lax.dot_general(wv[g], ckvn[...], NT, preferred_element_type=F32).astype(BF16)

    def score(b, u, q, k):
        cols, i, hd = slice(u // GH * seq, (u // GH + 1) * seq), u % GH, rd // 2
        cos_t, sin_t = rope_t[0:hd, :], rope_t[hd:rd, :]
        base = i * (128 + rd)
        fr = q[base + 128:base + 128 + hd, cols].astype(F32)
        bk = q[base + 128 + hd:base + 128 + rd, cols].astype(F32)
        q_cat = jnp.concatenate(
            [q[base:base + 128, cols], (fr * cos_t - bk * sin_t).astype(BF16), (fr * sin_t + bk * cos_t).astype(BF16)], axis=0
        )
        k_cat = jnp.concatenate([k[cols, i * 128:(i + 1) * 128], kpo[b % 2, cols, :]], axis=1)
        return jnp.dot(k_cat, q_cat, preferred_element_type=F32)

    def softmax(sc):
        sc = jnp.where(causal, sc, -jnp.inf)
        top = jnp.max(sc, axis=0, keepdims=True)
        e = jnp.exp2((sc - top) * (scale * LOG2E))
        return (e * (1.0 / jnp.sum(e, axis=0, keepdims=True))).astype(BF16)

    def attend(b, g, q, k, v):
        units = range(GH * BS)
        for u in units:
            scores[u] = score(b, u, q, k)
        for u in units:
            probs[u] = softmax(scores[u])
        for u in units:
            cols, i = slice(u // GH * seq, (u // GH + 1) * seq), u % GH
            o = jnp.dot(v[i * 128:(i + 1) * 128, cols], probs[u], preferred_element_type=F32)
            ctx[pl.ds(pl.multiple_of(g * (GH * 128) + i * 128, 128), 128), cols] = o.astype(BF16)

    def begin(b):
        @pl.when(b == 0)
        def _():
            for copy in weight_copies[1:]:
                copy.wait()

        project(0, qa, ka, va)

    def two(b, j):
        g = 2 * j
        project(g + 1, qb, kb, vb)
        attend(b, g, qa, ka, va)
        project(g + 2, qa, ka, va)
        attend(b, g + 1, qb, kb, vb)

    def finish(b):
        project(groups - 1, qb, kb, vb)
        attend(b, groups - 2, qa, ka, va)
        attend(b, groups - 1, qb, kb, vb)
        out_first(b)

    def out_first(b):
        @pl.when(b >= 2)
        def _():
            o1_copy(b - 2).wait_send()

        o1s[b % 2] = jnp.dot(wo[half:, :], ctx[...], preferred_element_type=F32).astype(BF16)
        o1_copy(b).start()
        own[b % 2] = jnp.dot(wo[:half, :], ctx[...], preferred_element_type=F32)

    def out_second(b):
        o1_copy(b).wait_recv()

        @pl.when(b >= 2)
        def _():
            o2_copy(b - 2).wait_send()

        o2s[b % 2] = (own[b % 2] + o1r[b % RING].astype(F32)).astype(BF16)
        o2_copy(b).start()
        hr_copy(b).start()

    def out_third(b):
        o2_copy(b).wait_recv()
        hr_copy(b).wait()

        @pl.when(b >= 2)
        def _():
            o3_copy(b - 2).wait()
            o3_local(b - 2).wait()

        both = o2s[b % 2].astype(F32) + o2r[b % RING].astype(F32)
        fin[b % 2] = (hres[b % 2].astype(F32) + jnp.transpose(both)).astype(BF16)
        o3_copy(b).start()
        o3_local(b).start()

    def step(n, carry):
        i = n - LEAD

        def stage(fn, b):
            pl.when(jnp.logical_and(b >= 0, b < nb))(lambda: fn(b))

        active = jnp.logical_and(i >= 0, i < nb)
        stage(reduce_z, i + 2)
        pl.when(i <= 0)(lambda: stage(down, i + LEAD))
        pl.when(jnp.logical_and(i >= 0, i + LEAD + 1 < nb))(lambda: down(i + LEAD + 1))
        chunks = width // 128
        for m in range(LEAD):
            @pl.when(n == m)
            def _():
                for j in range(chunks * m // LEAD, chunks * (m + 1) // LEAD):
                    turn(j)

        stage(normalize, i)
        pl.when(active)(lambda: begin(i))

        def pair(j, c):
            pl.when(active)(lambda: two(i, j))

            @pl.when(j == 0)
            def _():
                stage(out_third, i - 2)
                stage(out_second, i - 1)

            @pl.when(j == max(groups // 2 - 3, 0))
            def _():
                stage(forward, i + 1)

            @pl.when(j == groups // 2 - 2)
            def _():
                stage(fetch, i + 1)
                stage(spread, i + 2)

            return c

        lax.fori_loop(0, groups // 2 - 1, pair, 0)
        pl.when(active)(lambda: finish(i))
        return carry

    lax.fori_loop(0, nb + LEAD + 2, step, 0)

    for b in (nb - 2, nb - 1):
        for d in range(1, nz):
            rs_copy(b, d).wait_send()
            ag_copy(b, d).wait_send()
        o1_copy(b).wait_send()
        o2_copy(b).wait_send()
        o3_copy(b).wait()
        o3_local(b).wait()
        cko_copy(b).wait()
        kpo_copy(b).wait()


def run_kernel(h, ssq, g_in, gains, rope, rope_t, wd, wq, wk, wv, wo, scale, nz, q_lora, kv_lora):
    toks, width = h.shape
    seq, rd = rope.shape[0], rope_t.shape[0]
    nb = toks // (BS * seq)
    blk, half = BS * seq, width // 2
    piece = blk // nz
    lat = q_lora // 4 + kv_lora // 4
    latw = wd.shape[1]
    dims = (nb, seq, nz, width * nz, q_lora, kv_lora, scale)
    dma = lambda *s: pltpu.SemaphoreType.DMA(s)
    vm = lambda *s: pltpu.VMEM(s, BF16)
    vf = lambda *s: pltpu.VMEM(s, F32)
    vmem = pl.BlockSpec(memory_space=pltpu.VMEM)
    anyw = pl.BlockSpec(memory_space=pl.ANY)
    gr = GH * 128
    proj = lambda: [vm(wq.shape[1], blk), vm(blk, gr), vm(gr, blk)]
    shape = jax.ShapeDtypeStruct
    scratch = (
        [vm(*wd.shape), vm(*wq.shape), vm(*wk.shape), vm(*wv.shape), vm(*wo.shape[::-1])]
        + proj() + proj() + [vf(GH * BS, seq, seq), vm(GH * BS, seq, seq)]
        + [vm(wo.shape[0], blk), vm(blk, q_lora), vm(blk, kv_lora), vm(blk, latw), vm(3, blk, lat)]
        + [vm(2, blk, width), vm(2, blk, latw), vm(RING, nz - 1, piece, latw), vm(2, piece, latw)]
        + [vm(2, half, blk), vf(2, half, blk), vm(2, half, blk), vm(2, blk, half), vm(2, blk, half)]
        + [vm(RING, half, blk), vm(RING, half, blk), vm(2, blk, kv_lora // 4), vm(2, blk, rd)]
        + [vf(nz - 1, *ssq.shape), vf(3, *gains.shape), vf(*ssq.shape)]
        + [dma(6), dma(2), dma(2, nz - 1), dma(2, 3)]
        + [dma(nb, nz - 1)] * 4 + [dma(2)] + [dma(nb)] * 6
        + [dma(4)] + [dma(nb)] * 6 + [dma(2)] * 4
    )
    return pl.pallas_call(
        functools.partial(kernel, dims),
        out_shape=[
            shape((toks, width), BF16), shape((toks, kv_lora // 4), BF16), shape((toks, rd), BF16),
            shape((toks, latw), BF16), shape((3, toks, lat), BF16),
        ],
        in_specs=[anyw] + [vmem] * 5 + [anyw] * 5,
        out_specs=[anyw] * 5,
        scratch_shapes=scratch,
        compiler_params=pltpu.CompilerParams(collective_id=0, has_side_effects=True, vmem_limit_bytes=67_043_328),
        cost_estimate=pl.CostEstimate(flops=171_000_000_000, bytes_accessed=100_000_000, transcendentals=17_000_000),
        name="mla_block",
    )(h, ssq, g_in, gains, rope, rope_t, wd, wq, wk, wv, wo)


def pack_weights(w_uq, w_uk, w_uv, w_o):
    cdim, heads, qk = w_uq.shape
    kdim, _, nope = w_uk.shape
    groups = heads // GH
    wq = w_uq.transpose(1, 2, 0).reshape(groups, GH * qk, cdim)
    wk = w_uk.transpose(1, 2, 0).reshape(groups, GH * nope, kdim)
    wv = w_uv.transpose(1, 2, 0).reshape(groups, GH * w_uv.shape[2], kdim)
    wo = w_o.reshape(heads * w_o.shape[1], w_o.shape[2])
    return wq, wk, wv, wo


def solution(mesh):
    nz = mesh.shape["emb"]
    in_specs = (P("dp", None, "emb"), P("emb"), P("emb", "head"), P("head"), P("emb", "head"), P("head"), P("emb", None), P(None, "head", None), P(None, "head", None), P(None, "head", None), P("head", None, "emb"))
    out_specs = (P("dp", None, "emb"), P("dp", None, "head"), P("dp", None, None))

    def local_block(hidden, g_in, w_dq, g_q, w_dkv, g_kv, w_kr, w_uq, w_uk, w_uv, w_o):
        nseq, seq, width = hidden.shape
        rd = w_kr.shape[1]
        soft_scale = MSCALE * MSCALE / math.sqrt(w_uq.shape[2])
        wide = hidden.astype(F32)
        ssq = jnp.sum(wide * wide, axis=-1)
        cos_t, sin_t = rope_tables(seq, rd)
        pad = jnp.zeros((seq, 128 - rd), F32)
        rope = jnp.concatenate([cos_t, cos_t, pad, -sin_t, sin_t, pad], axis=1)
        rope_t = jnp.concatenate([cos_t, sin_t], axis=1).T
        gains = jnp.broadcast_to(jnp.concatenate([g_q, g_kv]).astype(F32)[None, :], (8, g_q.shape[0] + g_kv.shape[0]))
        gin = jnp.broadcast_to(g_in.astype(F32)[None, :], (8, width))
        wd = jnp.concatenate([w_dq, w_dkv, w_kr, jnp.zeros((width, 128 - rd), BF16)], axis=1)
        wq, wk, wv, wo = pack_weights(w_uq, w_uk, w_uv, w_o)
        toks = nseq * seq
        out, ckv, kpe = run_kernel(
            hidden.reshape(toks, width), ssq, gin, gains, rope, rope_t, wd, wq, wk, wv, wo,
            soft_scale, nz, w_uq.shape[0], w_uk.shape[0],
        )[:3]
        return out.reshape(hidden.shape), ckv.reshape(nseq, seq, -1), kpe.reshape(nseq, seq, rd)

    return jax.shard_map(local_block, mesh=mesh, in_specs=in_specs, out_specs=out_specs, check_vma=False)
```
